32 devices in a mesh: seq: 8 (over z, x), batch: 4 (over y, core).
Axes of the slice: x: 2, y: 2, z: 4, core: 2. Of those that a mesh axis runs over, the one named last changes fastest.
Arguments:
- hidden: bfloat16 [8, 2048, 4096], P('batch', None, 'seq')
- gain: float32 [4096], P('seq'), may hold values from 0.5 to 1.5
- value_weight: float32 [4096], P('seq'), may hold values from -0.09375 to 0.09375
- rewards: float32 [8, 2048], P('batch', 'seq'), may hold values from -1.5 to 1.5
- reward_mask: int32 [8, 2048], P('batch', 'seq'), may hold values 0 or 1
- lengths: int32 [8], P('batch'), may hold values from 512 to 2048
- horizon: float32 [8], P('batch'), may hold values from 24 to 16384
Outputs:
- advantages: float32 [8, 2048], P(None, ('seq', 'batch'))
- returns: float32 [8, 2048], P(None, ('seq', 'batch'))
The draws below stay inside these ranges and needn't reach their ends.
All inputs are finite; a program needn't handle non-finite values. No bound on the sum of `reward_mask` on one device may be relied on, other than what follows from the above.
Results may differ from the reference program's by a relative error of at most 0.0003.
Values may be sent and summed in bfloat16 or wider, within the bound.
A program may use at most 64 MiB of HBM per device.

```python
import jax
import jax.numpy as jnp
from jax import lax

D = 4096
B = 8
S = 2048


def draw_hidden(key, part):
    first_key = jax.random.fold_in(key, 11)
    second_key = jax.random.fold_in(key, 12)
    base = jax.random.normal(first_key, (B, S, D), jnp.float32)
    scales = jnp.exp(jax.random.uniform(second_key, (B, S, D // 16, 1), jnp.float32, -1.2, 1.2))
    return (base.reshape(B, S, D // 16, 16) * scales).reshape(B, S, D).astype(jnp.bfloat16)


def draw_horizon(key, part):
    inner = jax.random.fold_in(key, 21)
    lower = jnp.log(24.0)
    upper = jnp.log(4.0 * S)
    return jnp.exp(jax.random.uniform(inner, (B,), jnp.float32, lower, upper)).astype(jnp.float32)


def place_ends(drawn, rng, least, high):
    dims = drawn.shape
    index_at = [jax.random.randint(jax.random.fold_in(rng, axis), (), 0, dims[axis]) for axis in range(len(dims))]
    drawn = drawn.at[tuple(index_at)].set(least)
    longest = dims.index(max(dims))
    index_at[longest] = (index_at[longest] + 1) % dims[longest]
    return drawn.at[tuple(index_at)].set(high)


def level_of(key, dims, shards, low, high):
    factor_of = 1.0
    for axis_at, parts in shards:
        steps = jax.random.uniform(jax.random.fold_in(jax.random.fold_in(key, 6), axis_at), (parts,), jnp.float32, low / len(shards), high / len(shards))
        factor_of = factor_of * jnp.repeat(jnp.exp(steps), dims[axis_at] // parts).reshape((-1,) + (1,) * (len(dims) - 1 - axis_at))
    return factor_of


def normal_values(own_key, dims, scale, limit, split=(), held_as=jnp.bfloat16):
    result = scale * jax.random.normal(own_key, dims, jnp.float32)
    if split:
        result = result * level_of(own_key, dims, split, -0.22, 0.18)
    return jnp.clip(result, -limit, limit).astype(held_as)


def setup_inputs(seed: int = 0) -> dict:
    splits = jax.random.split(jax.random.key(seed), 8)
    return {
        "hidden": draw_hidden(jax.random.fold_in(splits[7], 71), 0),
        "gain": jnp.clip(1.0 + 0.1 * jax.random.normal(splits[1], (D,), jnp.float32), 0.5, 1.5),
        "value_weight": normal_values(splits[2], (D,), D ** -0.5, 0.09375, ((0, 8),), jnp.float32),
        "rewards": normal_values(splits[3], (B, S), 0.1, 1.5, ((0, 4), (1, 8)), jnp.float32),
        "reward_mask": place_ends((jax.random.randint(splits[4], (B, S), 0, 4) < 1).astype(jnp.int32), jax.random.fold_in(splits[4], 1), 0, 1),
        "lengths": place_ends(jax.random.randint(splits[5], (B,), S // 4, S + 1), jax.random.fold_in(splits[5], 1), S // 4, S).astype(jnp.int32),
        "horizon": draw_horizon(jax.random.fold_in(splits[7], 71), 0),
    }


EPS = 1e-05

def reference(hidden, gain, value_weight, rewards, reward_mask, lengths, horizon):
    head_vec = gain * value_weight

    def head(rows):
        wide_rows = rows.astype(jnp.float32)
        return lax.optimization_barrier(jnp.sum(wide_rows * head_vec, -1)) * lax.rsqrt(lax.optimization_barrier(jnp.mean(wide_rows * wide_rows, -1)) + EPS)
    values = lax.map(head, hidden)
    length_all = hidden.shape[1]
    positions = jnp.arange(length_all, dtype=jnp.int32)
    valid = (positions[None, :] < lengths[:, None]).astype(jnp.float32)
    next_valid = (positions[None, :] + 1 < lengths[:, None]).astype(jnp.float32)
    next_values = jnp.concatenate([values[:, 1:], jnp.zeros((values.shape[0], 1), jnp.float32)], 1)
    delta = (rewards * reward_mask.astype(jnp.float32) + next_valid * next_values - values) * valid
    decay = jnp.exp(-1.0 / horizon)

    def step(carry, inputs):
        d_now, v_next = inputs
        fresh = d_now + decay * v_next * carry
        return (fresh, fresh)
    _, gae_t = lax.scan(step, jnp.zeros(values.shape[0], jnp.float32), (delta.T, next_valid.T), reverse=True)
    gae = gae_t.T
    returns = (gae + values) * valid
    count = jnp.sum(valid)
    first = jnp.sum(gae)
    second = jnp.sum(gae * gae)
    mean = first / count
    var = jnp.maximum(second / count - mean * mean, 1.0)
    advantages = (gae - mean) * valid * lax.rsqrt(var)
    return (advantages, returns)
```

```python
import functools

import jax
import jax.numpy as jnp
from jax import lax
from jax.experimental import pallas as pl
from jax.experimental.pallas import tpu as pltpu
from jax.sharding import PartitionSpec as P

EPS = 1e-05
LANES = 128
F32 = jnp.float32


def kernel(n, nb, owners, hidden, gain, weight, rewards, mask, lengths, horizon,
           out_ref,
           hv, gain_v, weight_v, rew_v, mask_v, len_s, hor_s,
           part, rbuf, rw_send, rw_recv, len_send, len_recv, hor_send, hor_recv,
           sum_send, sum_recv, tok_send, tok_recv,
           chunk_sem, small_sem, part_ss, part_rs, rw_ss, rw_rs, info_ss, info_rs,
           sum_ss, sum_rs, tok_ss, tok_rs, sum_all, tok_all):
    R, T, depth = hidden.shape
    block = rewards.shape[1]
    width = block // nb
    per = n // owners
    base = (n - owners) // 2
    L = T // owners
    G = L // LANES
    gb = block // LANES
    rows = G * R
    total = depth * n
    s = lax.axis_index("seq")
    b = lax.axis_index("batch")
    is_owner = (s >= base) & (s < base + owners)
    mine = s - base
    out_o = s // per
    rw_at = base + out_o
    half = s % per

    def chunk_copy(o, r):
        span = pl.ds(o * L, L)
        return pltpu.make_async_copy(hidden.at[r, span, :], hv.at[r, span, :], chunk_sem.at[o, r])

    smalls = [
        pltpu.make_async_copy(src, dst, small_sem.at[i])
        for i, (src, dst) in enumerate(
            ((gain, gain_v), (weight, weight_v), (rewards, rew_v), (mask, mask_v),
             (lengths, len_s), (horizon, hor_s)))
    ]
    for copy in smalls:
        copy.start()
    near_high = s * (owners // 2) // n
    near_low = s % 2

    def turn(k):
        back = owners - 1 - k
        if owners % 2:
            return (s + back) % owners
        return (near_high + back // 2) % (owners // 2) * 2 + (near_low + back) % 2

    for k in range(owners):
        for r in range(R):
            chunk_copy(turn(k), r).start()
    barrier = pltpu.get_barrier_semaphore()
    for k in range(1, n):
        peer = (s + k) % n

        @pl.when(is_owner | ((peer >= base) & (peer < base + owners)))
        def _():
            pl.semaphore_signal(barrier, inc=1, device_id={"seq": peer},
                                device_id_type=pl.DeviceIdType.MESH)
    for k in range(1, nb):
        pl.semaphore_signal(barrier, inc=1, device_id={"batch": lax.rem(b + k, nb)},
                            device_id_type=pl.DeviceIdType.MESH)
    for copy in smalls:
        copy.wait()

    head = (gain_v[...] * weight_v[...]).reshape(1, depth)
    high = head.astype(jnp.bfloat16).astype(F32)
    middle = (head - high).astype(jnp.bfloat16).astype(F32)
    low = head - high - middle
    wrow = lax.broadcasted_iota(jnp.int32, (16, depth), 0)
    pieces = jnp.where(wrow == 0, high, jnp.where(wrow == 1, middle, jnp.where(wrow == 2, low, 0.0)))
    pieces = pieces.astype(jnp.bfloat16)

    rw = rew_v[...] * mask_v[...].astype(F32)
    for g in range(gb):
        rw_send[g * R:(g + 1) * R, :] = rw[:, g * LANES:(g + 1) * LANES]
    for r in range(R):
        len_send[r:r + 1, :] = jnp.full((1, LANES), len_s[r], jnp.int32)
        hor_send[r:r + 1, :] = jnp.full((1, LANES), hor_s[r], F32)

    infos = []
    for k in range(1, nb):
        for i, (src, dst) in enumerate(((len_send, len_recv), (hor_send, hor_recv))):
            infos.append((k, i, src, dst))

    def info_copy(k, i, src, dst):
        return pltpu.make_async_remote_copy(
            src, dst.at[b], info_ss.at[i], info_rs.at[i],
            device_id={"batch": lax.rem(b + k, nb)}, device_id_type=pl.DeviceIdType.MESH)

    def bytes_of(ref, sem):
        return pltpu.make_async_copy(ref, ref, sem)

    def part_copy(o):
        return pltpu.make_async_remote_copy(
            part.at[o], rbuf.at[s], part_ss, part_rs,
            device_id={"seq": base + o}, device_id_type=pl.DeviceIdType.MESH)

    def rw_copy():
        return pltpu.make_async_remote_copy(
            rw_send, rw_recv.at[half], rw_ss, rw_rs,
            device_id={"seq": rw_at}, device_id_type=pl.DeviceIdType.MESH)

    def send_part(o):
        @pl.when(base + o != s)
        def _():
            part_copy(o).start()

    meet = min(1, owners - 1)

    def compute(k, carry):
        o = turn(k)
        for r in range(R):
            chunk_copy(o, r).wait()
            for g in range(G):
                at = pl.ds(pl.multiple_of(o * L + g * LANES, LANES), LANES)
                h = hv[r, at, :]
                sums = lax.dot_general(pieces, h, (((1,), (1,)), ((), ())),
                                       preferred_element_type=F32)
                squares = jnp.zeros((LANES, LANES), F32)
                for j in range(depth // LANES):
                    wide = h[:, j * LANES:(j + 1) * LANES].astype(F32)
                    squares = squares + wide * wide
                row = g * R + r
                part[o, 0, row:row + 1, :] = jnp.sum(sums[0:8], 0, keepdims=True)
                part[o, 1, row:row + 1, :] = jnp.sum(squares.T, 0, keepdims=True)

        @pl.when(k == meet)
        def _():
            met = jnp.where(is_owner, n - 1, owners) + nb - 1
            pl.semaphore_wait(barrier, met)
            for before in range(meet):
                send_part(turn(before))

            @pl.when(rw_at != s)
            def _():
                rw_copy().start()

            for entry in infos:
                info_copy(*entry).start()

        @pl.when(k >= meet)
        def _():
            send_part(o)
        return carry

    lax.fori_loop(0, owners, compute, 0)

    @pl.when(rw_at == s)
    def _():
        rw_recv[half] = rw_send[...]

    len_recv[b] = len_send[...]
    hor_recv[b] = hor_send[...]

    def sum_copy(i, j):
        return pltpu.make_async_remote_copy(
            sum_send, sum_recv.at[mine, b], sum_ss, sum_rs,
            device_id={"seq": i, "batch": j}, device_id_type=pl.DeviceIdType.MESH)

    def each_sum(act):
        def one(i):
            for j in range(nb):
                if isinstance(i, int) and not base <= i < base + owners:
                    act(sum_copy(i, j))
                else:
                    @pl.when((i != s) | (j != b))
                    def _():
                        act(sum_copy(i, j))

        if n * nb <= 32:
            for i in range(n):
                one(i)
        else:
            def body(i, carry):
                one(i)
                return carry
            lax.fori_loop(0, n, body, 0)

    def tok_copy(h, j):
        c = lax.rem(b + j, nb)
        g = h * gb + (c * width) // LANES
        return pltpu.make_async_remote_copy(
            tok_send.at[g], tok_recv.at[b], tok_ss, tok_rs,
            device_id={"seq": mine * per + h, "batch": c}, device_id_type=pl.DeviceIdType.MESH)

    def tok_local(h):
        g = h * gb + (b * width) // LANES
        tok_recv[b] = tok_send[g]

    @pl.when(is_owner)
    def _():
        row = lax.broadcasted_iota(jnp.int32, (rows, LANES), 0)
        lane = lax.broadcasted_iota(jnp.int32, (rows, LANES), 1)
        group = row // R
        which = row % R
        length = jnp.full((rows, LANES), len_s[0], jnp.int32)
        reach = jnp.full((rows, LANES), hor_s[0], F32)
        for r in range(1, R):
            length = jnp.where(which == r, len_s[r], length)
            reach = jnp.where(which == r, hor_s[r], reach)
        rate = -1.0 / reach
        local = group * LANES + lane
        token = mine * L + local
        valid = (token < length).astype(F32)
        next_valid = (token + 1 < length).astype(F32)
        levels = [[j * k for j in range(1, min(8, LANES // k))] for k in (1, 8, 64)]
        lane_decay = [[jnp.where(lane < LANES - k, jnp.exp(rate * k), 0.0) for k in level]
                      for level in levels]
        hops = [1 << i for i in range(max(G - 1, 0).bit_length())]
        row_decay = [jnp.where(group + k < G, jnp.exp(rate * (k * LANES)), 0.0) for k in hops]
        into = jnp.where(group < G - 1, jnp.exp(rate * (LANES - lane).astype(F32)), 0.0)
        power = jnp.exp(rate * (L - 1 - local).astype(F32))
        decay = jnp.exp(rate)
        power_sum = jnp.sum(power, 1, keepdims=True)
        power_squares = jnp.sum(power * power, 1, keepdims=True)

        @pl.when(s // per == mine)
        def _():
            if per > 1:
                bytes_of(rw_recv.at[pl.ds(0, per - 1)], rw_rs).wait()

        @pl.when(s // per != mine)
        def _():
            bytes_of(rw_recv, rw_rs).wait()
        gains = jnp.concatenate([rw_recv[h] for h in range(per)], 0)

        rbuf[s] = part[mine]
        bytes_of(rbuf.at[pl.ds(0, n - 1)], part_rs).wait()
        projected = rbuf[0, 0]
        squares = rbuf[0, 1]
        for k in range(1, n):
            projected = projected + rbuf[k, 0]
            squares = squares + rbuf[k, 1]
        values = projected * lax.rsqrt(squares / total + EPS)
        ahead = pltpu.roll(values, LANES - 1, 1)
        if G > 1:
            after = jnp.where(group < G - 1, pltpu.roll(ahead, rows - R, 0), 0.0)
        else:
            after = jnp.zeros_like(ahead)
        next_values = jnp.where(lane == LANES - 1, after, ahead)
        gae = (gains + next_valid * next_values - values) * valid
        for level, factors in zip(levels, lane_decay):
            terms = [factor * pltpu.roll(gae, LANES - k, 1) for k, factor in zip(level, factors)]
            gae = gae + sum(terms[1:], terms[0])
        if G > 1:
            start = jnp.broadcast_to(gae[:, 0:1], (rows, LANES))
            for k, factor in zip(hops, row_decay):
                start = start + factor * pltpu.roll(start, rows - k * R, 0)
            gae = gae + into * pltpu.roll(start, rows - R, 0)
        for g in range(G):
            tok_send[g, 0] = gae[g * R:(g + 1) * R]
            tok_send[g, 1] = values[g * R:(g + 1) * R]
        sums = jnp.where(lane == 1, jnp.sum(gae, 1, keepdims=True), 0.0)
        sums = jnp.where(lane == 2, 2.0 * jnp.sum(gae * power, 1, keepdims=True), sums)
        sums = jnp.where(lane == 3, jnp.sum(gae * gae, 1, keepdims=True), sums)
        sums = jnp.where(lane == 4, power_sum, sums)
        sums = jnp.where(lane == 5, power_squares, sums)
        sums = jnp.where((lane == 0) & (group == 0), values + decay * gae, sums)
        summary = sums[0:R]
        for g in range(1, G):
            summary = summary + sums[g * R:(g + 1) * R]
        sum_send[...] = summary
        sum_recv[mine, b] = summary
        each_sum(lambda copy: copy.start())
        for h in range(per):
            for j in range(1, nb):
                tok_copy(h, j).start()

            @pl.when(mine * per + h == s)
            def _():
                tok_local(h)

            @pl.when(mine * per + h != s)
            def _():
                tok_copy(h, 0).start()

    @pl.when(is_owner)
    def _():
        bytes_of(part.at[pl.ds(0, owners - 1)], part_ss).wait()

    @pl.when(jnp.logical_not(is_owner))
    def _():
        bytes_of(part, part_ss).wait()

    @pl.when(rw_at != s)
    def _():
        rw_copy().wait_send()

    for i, dst in enumerate((len_recv, hor_recv)):
        bytes_of(dst.at[pl.ds(0, nb - 1)], info_ss.at[i]).wait()
        bytes_of(dst.at[pl.ds(0, nb - 1)], info_rs.at[i]).wait()
    lane = lax.broadcasted_iota(jnp.int32, (R, LANES), 1)
    group_out = half * gb + (b * width) // LANES
    local = group_out * LANES + lane
    token = out_o * L + local
    count = jnp.zeros((R, LANES), F32)
    jump, power_out, valid_out, lens = [], [], [], []
    for c in range(nb):
        length = len_recv[c]
        rate = -1.0 / hor_recv[c]
        count = count + jnp.minimum(length, T).astype(F32)
        jump.append(jnp.exp(rate * float(L)))
        power_out.append(jnp.exp(rate * (L - 1 - local).astype(F32)))
        valid_out.append((token < length).astype(F32))
        lens.append(length)
    count = jnp.sum(count, 0, keepdims=True)

    @pl.when(is_owner)
    def _():
        bytes_of(sum_all.at[pl.ds(0, n * nb - 1)], sum_ss).wait()

        @pl.when(s // per == mine)
        def _():
            bytes_of(tok_all.at[pl.ds(0, per * nb - 1)], tok_ss).wait()

        @pl.when(s // per != mine)
        def _():
            bytes_of(tok_all, tok_ss).wait()

    @pl.when(is_owner)
    def _():
        bytes_of(sum_all.at[pl.ds(0, owners * nb - 1)], sum_rs).wait()

    @pl.when(jnp.logical_not(is_owner))
    def _():
        bytes_of(sum_recv, sum_rs).wait()

    acc = jnp.zeros((R, LANES), F32)
    entering = []
    for c in range(nb):
        u = jnp.zeros((R, LANES), F32)
        chosen = jnp.zeros((R, LANES), F32)
        for o in reversed(range(owners)):
            message = sum_recv[o, c]
            factor = jnp.where((lane == 1) | (lane == 3), 1.0,
                               jnp.where((lane == 2) | (lane == 4), u,
                                         jnp.where(lane == 5, u * u, 0.0)))
            acc = acc + message * factor
            chosen = jnp.where(out_o == o, u, chosen)
            if o:
                first_value = jnp.broadcast_to(message[:, 0:1], (R, LANES))
                u = jnp.where(o * L < lens[c], first_value + jump[c] * u, 0.0)
        entering.append(chosen)
    acc = jnp.sum(acc, 0, keepdims=True)
    lane1 = lax.broadcasted_iota(jnp.int32, (1, LANES), 1)
    first = jnp.sum(jnp.where((lane1 == 1) | (lane1 == 4), acc, 0.0), 1, keepdims=True)
    second = jnp.sum(jnp.where((lane1 == 2) | (lane1 == 3) | (lane1 == 5), acc, 0.0), 1, keepdims=True)
    mean = first / count
    var = jnp.maximum(second / count - mean * mean, 1.0)
    scale = lax.rsqrt(var)

    @pl.when(rw_at == s)
    def _():
        bytes_of(tok_recv.at[pl.ds(0, nb - 1)], tok_rs).wait()

    @pl.when(rw_at != s)
    def _():
        bytes_of(tok_recv, tok_rs).wait()
    spots = LANES // width
    spot = b % spots

    def pick(x):
        result = x[:, 0:width]
        for j in range(1, spots):
            result = jnp.where(spot == j, x[:, j * width:(j + 1) * width], result)
        return result

    for c in range(nb):
        gae = tok_recv[c, 0] + power_out[c] * entering[c]
        out_ref[(nb + c) * R:(nb + c + 1) * R, :] = pick((gae + tok_recv[c, 1]) * valid_out[c])
        out_ref[c * R:(c + 1) * R, :] = pick((gae - mean) * valid_out[c] * scale)


def per_device(hidden, gain, weight, rewards, mask, lengths, horizon):
    n = lax.axis_size("seq")
    nb = lax.axis_size("batch")
    owners = n // 2 if n % 4 == 0 else n
    R, T, depth = hidden.shape
    block = rewards.shape[1]
    per = n // owners
    G = T // owners // LANES
    gb = block // LANES
    rows = G * R
    dma = pltpu.SemaphoreType.DMA
    both = pl.pallas_call(
        functools.partial(kernel, n, nb, owners),
        out_shape=pltpu.VMEM((2 * R * nb, block // nb), F32),
        in_specs=[pl.BlockSpec(memory_space=pl.ANY)] * 7,
        out_specs=pl.BlockSpec(memory_space=pltpu.VMEM),
        scratch_shapes=[
            pltpu.VMEM((R, T, depth), jnp.bfloat16),
            pltpu.VMEM((depth,), F32),
            pltpu.VMEM((depth,), F32),
            pltpu.VMEM((R, block), F32),
            pltpu.VMEM((R, block), jnp.int32),
            pltpu.SMEM((R,), jnp.int32),
            pltpu.SMEM((R,), F32),
            pltpu.VMEM((owners, 2, rows, LANES), F32),
            pltpu.VMEM((n, 2, rows, LANES), F32),
            pltpu.VMEM((gb * R, LANES), F32),
            pltpu.VMEM((per, gb * R, LANES), F32),
            pltpu.VMEM((R, LANES), jnp.int32),
            pltpu.VMEM((nb, R, LANES), jnp.int32),
            pltpu.VMEM((R, LANES), F32),
            pltpu.VMEM((nb, R, LANES), F32),
            pltpu.VMEM((R, LANES), F32),
            pltpu.VMEM((owners, nb, R, LANES), F32),
            pltpu.VMEM((G, 2, R, LANES), F32),
            pltpu.VMEM((nb, 2, R, LANES), F32),
            dma((owners, R)), dma((6,)),
            dma(()), dma(()),
            dma(()), dma(()),
            dma((2,)), dma((2,)),
            dma(()), dma(()),
            dma(()), dma(()),
            pltpu.VMEM((n * nb, R, LANES), F32),
            pltpu.VMEM((per * nb, 2, R, LANES), F32),
        ],
        compiler_params=pltpu.CompilerParams(collective_id=0, has_side_effects=True),
    )(hidden, gain, weight, rewards, mask, lengths, horizon)
    return both[:R * nb], both[R * nb:]


def solution(mesh):
    return jax.shard_map(
        per_device,
        mesh=mesh,
        in_specs=(
            P("batch", None, "seq"),
            P("seq"),
            P("seq"),
            P("batch", "seq"),
            P("batch", "seq"),
            P("batch"),
            P("batch"),
        ),
        out_specs=(P(None, ("seq", "batch")), P(None, ("seq", "batch"))),
        check_vma=False,
    )
```

```python
import functools

import jax
import jax.numpy as jnp
from jax import lax
from jax.experimental import pallas as pl
from jax.experimental.pallas import tpu as pltpu
from jax.sharding import PartitionSpec as P

EPS = 1e-05
LANES = 128
F32 = jnp.float32
MESH = pl.DeviceIdType.MESH


def bytes_of(ref, sem):
    return pltpu.make_async_copy(ref, ref, sem)


def stack(pieces):
    return pieces[0] if len(pieces) == 1 else jnp.concatenate(pieces, 0)


def kernel(n, nb, pair, owners, hidden, gain, weight, rewards, mask, lengths, horizon,
           out_ref,
           hv, gain_v, weight_v, rew_v, mask_v, len_s, hor_s,
           part, rbuf, rw_send, rw_recv, len_send, len_recv, hor_send, hor_recv,
           sum_send, sum_recv, tok_send, tok_recv, sum_all, tok_all,
           chunk_sem, small_sem, part_ss, part_rs, rw_ss, rw_rs, info_ss, info_rs,
           sum_ss, sum_rs, tok_ss, tok_rs):
    R, T, depth = hidden.shape
    block = rewards.shape[1]
    width = block // nb
    per = n // owners
    base = (n - owners) // 2
    L = T // owners
    G = L // LANES
    gb = block // LANES
    rows = G * R
    Q = pair * R
    pairs = nb // pair
    total = depth * n
    s = lax.axis_index("seq")
    b = lax.axis_index("batch")
    side = b % pair
    mate = b // pair
    lead = mate * pair + pair - 1
    is_owner = (s >= base) & (s < base + owners) & (side == pair - 1)
    mine = s - base
    out_o = s // per
    half = s % per
    rw_at = base + out_o

    def chunk_copy(o):
        span = pl.ds(o * L, L)
        return pltpu.make_async_copy(hidden.at[:, span, :], hv.at[:, span, :], chunk_sem.at[o])

    smalls = [
        pltpu.make_async_copy(src, dst, small_sem.at[i])
        for i, (src, dst) in enumerate(
            ((gain, gain_v), (weight, weight_v), (rewards, rew_v), (mask, mask_v),
             (lengths, len_s), (horizon, hor_s)))
    ]
    for copy in smalls:
        copy.start()
    near_high = s * (owners // 2) // n
    near_low = s % 2

    def turn(k):
        back = owners - 1 - k
        if owners % 2:
            return (s + back) % owners
        return (near_high + back // 2) % (owners // 2) * 2 + (near_low + back) % 2

    for k in range(owners):
        chunk_copy(turn(k)).start()
    barrier = pltpu.get_barrier_semaphore()
    for k in range(1, nb):
        pl.semaphore_signal(barrier, inc=1, device_id={"batch": lax.rem(b + k, nb)},
                            device_id_type=MESH)

    @pl.when(is_owner)
    def _():
        for k in range(n):
            for c in range(pair):
                if k or c:
                    pl.semaphore_signal(
                        barrier, inc=1,
                        device_id={"seq": (s + k) % n, "batch": mate * pair + (side + c) % pair},
                        device_id_type=MESH)

    smalls[0].wait()
    smalls[1].wait()
    head = (gain_v[...] * weight_v[...]).reshape(1, depth)
    high = head.astype(jnp.bfloat16).astype(F32)
    middle = (head - high).astype(jnp.bfloat16).astype(F32)
    low = head - high - middle
    wrow = lax.broadcasted_iota(jnp.int32, (16, depth), 0)
    pieces = jnp.where(wrow == 0, high, jnp.where(wrow == 1, middle, jnp.where(wrow == 2, low, 0.0)))
    pieces = pieces.astype(jnp.bfloat16)

    def part_copy(o):
        return pltpu.make_async_remote_copy(
            part.at[o], rbuf.at[s * pair + side], part_ss, part_rs,
            device_id={"seq": base + o, "batch": lead}, device_id_type=MESH)

    def rw_copy():
        return pltpu.make_async_remote_copy(
            rw_send, rw_recv.at[side * per + half], rw_ss, rw_rs,
            device_id={"seq": rw_at, "batch": lead}, device_id_type=MESH)

    def info_copy(k, i, src, dst):
        return pltpu.make_async_remote_copy(
            src, dst.at[b], info_ss.at[i], info_rs.at[i],
            device_id={"batch": lax.rem(b + k, nb)}, device_id_type=MESH)

    infos = ((len_send, len_recv), (hor_send, hor_recv))
    own_rw = is_owner & (mine == out_o)

    def send_part(o):
        @pl.when(jnp.logical_not(is_owner & (mine == o)))
        def _():
            part_copy(o).start()

    meet = min(1, owners - 1)

    def compute(k, carry):
        o = turn(k)
        chunk_copy(o).wait()
        for g in range(G):
            for r in range(R):
                at = pl.ds(pl.multiple_of(o * L + g * LANES, LANES), LANES)
                h = hv[r, at, :]
                sums = lax.dot_general(pieces, h, (((1,), (1,)), ((), ())),
                                       preferred_element_type=F32)
                squares = jnp.zeros((LANES, LANES), F32)
                for j in range(depth // LANES):
                    wide = h[:, j * LANES:(j + 1) * LANES].astype(F32)
                    squares = squares + wide * wide
                row = g * R + r
                part[o, 0, row:row + 1, :] = jnp.sum(sums[0:8], 0, keepdims=True)
                part[o, 1, row:row + 1, :] = jnp.sum(squares.T, 0, keepdims=True)

        @pl.when(k == meet)
        def _():
            for copy in smalls[2:]:
                copy.wait()
            rw = rew_v[...] * mask_v[...].astype(F32)
            for g in range(gb):
                rw_send[g * R:(g + 1) * R, :] = rw[:, g * LANES:(g + 1) * LANES]
            for r in range(R):
                len_send[r:r + 1, :] = jnp.full((1, LANES), len_s[r], jnp.int32)
                hor_send[r:r + 1, :] = jnp.full((1, LANES), hor_s[r], F32)
            met = jnp.where(is_owner, owners - 1, owners) + nb - 1
            pl.semaphore_wait(barrier, met)
            for before in range(meet):
                send_part(turn(before))

            @pl.when(jnp.logical_not(own_rw))
            def _():
                rw_copy().start()

            for j in range(1, nb):
                for i, (src, dst) in enumerate(infos):
                    info_copy(j, i, src, dst).start()

        @pl.when(k >= meet)
        def _():
            send_part(o)
        return carry

    lax.fori_loop(0, owners, compute, 0)

    @pl.when(own_rw)
    def _():
        rw_recv[side * per + half] = rw_send[...]

    len_recv[b] = len_send[...]
    hor_recv[b] = hor_send[...]
    for i, (src, dst) in enumerate(infos):
        bytes_of(dst.at[pl.ds(0, nb - 1)], info_rs.at[i]).wait()

    def sum_copy(i, j):
        return pltpu.make_async_remote_copy(
            sum_send, sum_recv.at[mine * pairs + mate], sum_ss, sum_rs,
            device_id={"seq": i, "batch": j}, device_id_type=MESH)

    def each_sum():
        def one(i):
            for j in range(nb):
                never = isinstance(i, int) and not base <= i < base + owners
                if never or j % pair != pair - 1:
                    sum_copy(i, j).start()
                else:
                    @pl.when((i != s) | (j != b))
                    def _():
                        sum_copy(i, j).start()

        if n * nb <= 32:
            for i in range(n):
                one(i)
        else:
            def body(i, carry):
                one(i)
                return carry
            lax.fori_loop(0, n, body, 0)

    def tok_copy(h, j):
        return pltpu.make_async_remote_copy(
            tok_send.at[h * gb + (j * width) // LANES], tok_recv.at[mate], tok_ss, tok_rs,
            device_id={"seq": mine * per + h, "batch": j}, device_id_type=MESH)

    @pl.when(is_owner)
    def _():
        row = lax.broadcasted_iota(jnp.int32, (pair * rows, LANES), 0)
        lane = lax.broadcasted_iota(jnp.int32, (pair * rows, LANES), 1)
        group = row % rows // R
        length = stack([len_recv[mate * pair + c] for c in range(pair) for _ in range(G)])
        reach = stack([hor_recv[mate * pair + c] for c in range(pair) for _ in range(G)])
        rate = -1.0 / reach
        local = group * LANES + lane
        valid = (mine * L + local < length).astype(F32)
        step = 16
        near = [jnp.where(lane < LANES - k, jnp.exp(rate * (k - 1)), 0.0) for k in range(1, step + 1)]
        far = [jnp.where(lane < LANES - k, jnp.exp(rate * k), 0.0) for k in range(step, LANES, step)]
        lead_in = jnp.exp(rate * lane.astype(F32))
        hops = [1 << i for i in range(max(G - 1, 0).bit_length())]
        row_decay = [jnp.where(group + k < G, jnp.exp(rate * (k * LANES)), 0.0) for k in hops]
        into = jnp.where(group < G - 1, jnp.exp(rate * (LANES - 1 - lane).astype(F32)), 0.0)
        power = jnp.exp(rate * (L - 1 - local).astype(F32))
        decay = jnp.exp(rate)
        power_sum = jnp.sum(power, 1, keepdims=True)
        power_squares = jnp.sum(power * power, 1, keepdims=True)
        fixed = jnp.where(lane == 4, power_sum, jnp.where(lane == 5, power_squares, 0.0))

        @pl.when(own_rw)
        def _():
            if pair * per > 1:
                bytes_of(rw_recv.at[pl.ds(0, pair * per - 1)], rw_rs).wait()

        @pl.when(jnp.logical_not(own_rw))
        def _():
            bytes_of(rw_recv, rw_rs).wait()
        gains = stack([rw_recv[c * per + h] for c in range(pair) for h in range(per)])

        rbuf[s * pair + side] = part[mine]
        bytes_of(rbuf.at[pl.ds(0, n * pair - 1)], part_rs).wait()
        projected, squares = [], []
        for c in range(pair):
            first, second = rbuf[c, 0], rbuf[c, 1]
            for k in range(1, n):
                first = first + rbuf[k * pair + c, 0]
                second = second + rbuf[k * pair + c, 1]
            projected.append(first)
            squares.append(second)
        values = stack(projected) * lax.rsqrt(stack(squares) / total + EPS)
        held = values * valid
        change = (gains - values) * valid
        mixed = decay * change + held
        start = jnp.sum(lead_in * mixed, 1, keepdims=True)
        terms = [factor * pltpu.roll(mixed if k < step else held, LANES - k, 1)
                 for k, factor in enumerate(near, 1)]
        while len(terms) > 1:
            terms = [sum(terms[i + 1:i + 2], terms[i]) for i in range(0, len(terms), 2)]
        gae = change + terms[0]
        terms = [factor * pltpu.roll(gae, LANES - k * step, 1) for k, factor in enumerate(far, 1)]
        while len(terms) > 1:
            terms = [sum(terms[i + 1:i + 2], terms[i]) for i in range(0, len(terms), 2)]
        gae = gae + terms[0]
        start = jnp.broadcast_to(start, gae.shape)
        if G > 1:
            for k, factor in zip(hops, row_decay):
                start = start + factor * pltpu.roll(start, pair * rows - k * R, 0)
            gae = gae + into * pltpu.roll(start, pair * rows - R, 0)
        sums = jnp.where(lane == 1, jnp.sum(gae, 1, keepdims=True), fixed)
        sums = jnp.where(lane == 2, 2.0 * jnp.sum(gae * power, 1, keepdims=True), sums)
        sums = jnp.where(lane == 3, jnp.sum(gae * gae, 1, keepdims=True), sums)
        sums = jnp.where((lane == 0) & (group == 0), start, sums)
        for c in range(pair):
            summary = sums[c * rows:c * rows + R]
            for g in range(1, G):
                summary = summary + sums[c * rows + g * R:c * rows + (g + 1) * R]
            sum_send[c * R:(c + 1) * R, :] = summary
        sum_recv[mine * pairs + mate] = sum_send[...]
        each_sum()
        for g in range(G):
            for c in range(pair):
                at = c * rows + g * R
                tok_send[g, 0, c * R:(c + 1) * R, :] = gae[at:at + R]
                tok_send[g, 1, c * R:(c + 1) * R, :] = values[at:at + R]
        for h in range(per):
            for j in range(nb):
                if j % pair != pair - 1:
                    tok_copy(h, j).start()
                else:
                    @pl.when((mine * per + h != s) | (j != b))
                    def _():
                        tok_copy(h, j).start()

                    @pl.when((mine * per + h == s) & (j == b))
                    def _():
                        tok_recv[mate] = tok_send[h * gb + (j * width) // LANES]

    @pl.when(is_owner)
    def _():
        if owners > 1:
            bytes_of(part.at[pl.ds(0, owners - 1)], part_ss).wait()

    @pl.when(jnp.logical_not(is_owner))
    def _():
        bytes_of(part, part_ss).wait()

    @pl.when(jnp.logical_not(own_rw))
    def _():
        rw_copy().wait_send()

    for i, (src, dst) in enumerate(infos):
        bytes_of(dst.at[pl.ds(0, nb - 1)], info_ss.at[i]).wait()

    spots = LANES // width
    spot = b % spots

    def pick(x):
        result = x[:, 0:width]
        for j in range(1, spots):
            result = jnp.where(spot == j, x[:, j * width:(j + 1) * width], result)
        return result

    every = nb * R
    lane = lax.broadcasted_iota(jnp.int32, (every, LANES), 1)
    local = (half * gb + (b * width) // LANES) * LANES + lane
    length = stack([len_recv[c] for c in range(nb)])
    rate = -1.0 / stack([hor_recv[c] for c in range(nb)])
    count = jnp.sum(jnp.minimum(length, T).astype(F32), 0, keepdims=True)
    jump = jnp.exp(rate * float(L))
    power_out = pick(jnp.exp(rate * (L - 1 - local).astype(F32)))
    valid_out = pick((out_o * L + local < length).astype(F32))

    @pl.when(is_owner)
    def _():
        bytes_of(sum_all.at[pl.ds(0, n * nb - 1)], sum_ss).wait()

    @pl.when(own_rw)
    def _():
        bytes_of(tok_all.at[pl.ds(0, per * nb - 1)], tok_ss).wait()

    @pl.when(is_owner & jnp.logical_not(own_rw))
    def _():
        bytes_of(tok_all, tok_ss).wait()

    @pl.when(is_owner)
    def _():
        bytes_of(sum_all.at[pl.ds(0, owners * pairs - 1)], sum_rs).wait()

    @pl.when(jnp.logical_not(is_owner))
    def _():
        bytes_of(sum_recv, sum_rs).wait()

    @pl.when(own_rw)
    def _():
        if pairs > 1:
            bytes_of(tok_recv.at[pl.ds(0, pairs - 1)], tok_rs).wait()

    @pl.when(jnp.logical_not(own_rw))
    def _():
        bytes_of(tok_recv, tok_rs).wait()

    gae = pick(stack([tok_recv[c, 0] for c in range(pairs)]))
    values = pick(stack([tok_recv[c, 1] for c in range(pairs)]))
    acc = jnp.zeros((every, LANES), F32)
    u = jnp.zeros((every, LANES), F32)
    entering = jnp.zeros((every, LANES), F32)
    for o in reversed(range(owners)):
        message = stack([sum_recv[o * pairs + c] for c in range(pairs)])
        factor = jnp.where((lane == 1) | (lane == 3), 1.0,
                           jnp.where((lane == 2) | (lane == 4), u,
                                     jnp.where(lane == 5, u * u, 0.0)))
        acc = acc + message * factor
        entering = jnp.where(out_o == o, u, entering)
        if o:
            u = jnp.broadcast_to(message[:, 0:1], (every, LANES)) + jump * u
    acc = jnp.sum(acc, 0, keepdims=True)
    lane1 = lax.broadcasted_iota(jnp.int32, (1, LANES), 1)
    first = jnp.sum(jnp.where((lane1 == 1) | (lane1 == 4), acc, 0.0), 1, keepdims=True)
    second = jnp.sum(jnp.where((lane1 == 2) | (lane1 == 3) | (lane1 == 5), acc, 0.0), 1, keepdims=True)
    mean = first / count[:, 0:1]
    var = jnp.maximum(second / count[:, 0:1] - mean * mean, 1.0)
    scale = lax.rsqrt(var)
    gae = gae + power_out * entering[:, 0:width]
    out_ref[every:2 * every, :] = (gae + values) * valid_out
    out_ref[0:every, :] = (gae - mean) * valid_out * scale


def per_device(hidden, gain, weight, rewards, mask, lengths, horizon):
    n = lax.axis_size("seq")
    nb = lax.axis_size("batch")
    pair = 2 - nb % 2
    owners = n // 2 if n % 4 == 0 else n
    R, T, depth = hidden.shape
    block = rewards.shape[1]
    per = n // owners
    G = T // owners // LANES
    gb = block // LANES
    rows = G * R
    Q = pair * R
    pairs = nb // pair
    dma = pltpu.SemaphoreType.DMA
    both = pl.pallas_call(
        functools.partial(kernel, n, nb, pair, owners),
        out_shape=pltpu.VMEM((2 * R * nb, block // nb), F32),
        in_specs=[pl.BlockSpec(memory_space=pl.ANY)] * 7,
        out_specs=pl.BlockSpec(memory_space=pltpu.VMEM),
        scratch_shapes=[
            pltpu.VMEM((R, T, depth), jnp.bfloat16),
            pltpu.VMEM((depth,), F32),
            pltpu.VMEM((depth,), F32),
            pltpu.VMEM((R, block), F32),
            pltpu.VMEM((R, block), jnp.int32),
            pltpu.SMEM((R,), jnp.int32),
            pltpu.SMEM((R,), F32),
            pltpu.VMEM((owners, 2, rows, LANES), F32),
            pltpu.VMEM((n * pair, 2, rows, LANES), F32),
            pltpu.VMEM((gb * R, LANES), F32),
            pltpu.VMEM((pair * per, gb * R, LANES), F32),
            pltpu.VMEM((R, LANES), jnp.int32),
            pltpu.VMEM((nb, R, LANES), jnp.int32),
            pltpu.VMEM((R, LANES), F32),
            pltpu.VMEM((nb, R, LANES), F32),
            pltpu.VMEM((Q, LANES), F32),
            pltpu.VMEM((owners * pairs, Q, LANES), F32),
            pltpu.VMEM((G, 2, Q, LANES), F32),
            pltpu.VMEM((pairs, 2, Q, LANES), F32),
            pltpu.VMEM((n * nb, Q, LANES), F32),
            pltpu.VMEM((per * nb, 2, Q, LANES), F32),
            dma((owners,)), dma((6,)),
            dma(()), dma(()),
            dma(()), dma(()),
            dma((2,)), dma((2,)),
            dma(()), dma(()),
            dma(()), dma(()),
        ],
        compiler_params=pltpu.CompilerParams(collective_id=0, has_side_effects=True),
    )(hidden, gain, weight, rewards, mask, lengths, horizon)
    return both[:R * nb], both[R * nb:]


def solution(mesh):
    return jax.shard_map(
        per_device,
        mesh=mesh,
        in_specs=(
            P("batch", None, "seq"),
            P("seq"),
            P("seq"),
            P("batch", "seq"),
            P("batch", "seq"),
            P("batch"),
            P("batch"),
        ),
        out_specs=(P(None, ("seq", "batch")), P(None, ("seq", "batch"))),
        check_vma=False,
    )
```

```python
import functools

import jax
import jax.numpy as jnp
from jax import lax
from jax.experimental import pallas as pl
from jax.experimental.pallas import tpu as pltpu
from jax.sharding import PartitionSpec as P

EPS = 1e-05
LANES = 128
TILE = 256
F32 = jnp.float32
MESH = pl.DeviceIdType.MESH


def bytes_of(ref, sem):
    return pltpu.make_async_copy(ref, ref, sem)


def stack(pieces):
    return pieces[0] if len(pieces) == 1 else jnp.concatenate(pieces, 0)


def kernel(n, nb, pair, owners, subs, hidden, gain, weight, rewards, mask, lengths, horizon,
           out_ref,
           hv, gain_v, weight_v, rew_v, mask_v, len_s, hor_s,
           part, rbuf, rw_send, rw_recv, len_send, len_recv, hor_send, hor_recv,
           sum_send, sum_recv, tok_send, tok_recv, sum_all, tok_all, held_squares,
           chunk_sem, small_sem, part_ss, part_rs, rw_ss, rw_rs, info_ss, info_rs,
           sum_ss, sum_rs, tok_ss, tok_rs):
    R, T, depth = hidden.shape
    block = rewards.shape[1]
    width = block // nb
    per = n // owners
    base = (n - owners) // 2
    L = T // owners
    G = L // LANES
    gb = block // LANES
    rows = G * R
    Q = pair * R
    pairs = nb // pair
    total = depth * n
    s = lax.axis_index("seq")
    b = lax.axis_index("batch")
    side = b % pair
    mate = b // pair
    lead = mate * pair + pair - 1
    is_owner = (s >= base) & (s < base + owners) & (side == pair - 1)
    mine = s - base
    out_o = s // per
    half = s % per
    rw_at = base + out_o

    S = L // subs

    def chunk_copy(o, j):
        span = pl.ds(o * L + j * S, S)
        return pltpu.make_async_copy(hidden.at[:, span, :], hv.at[:, span, :], chunk_sem.at[o, j])

    smalls = [
        pltpu.make_async_copy(src, dst, small_sem.at[i])
        for i, (src, dst) in enumerate(
            ((gain, gain_v), (weight, weight_v), (rewards, rew_v), (mask, mask_v),
             (lengths, len_s), (horizon, hor_s)))
    ]
    for copy in smalls:
        copy.start()
    near_high = s * (owners // 2) // n
    near_low = s % 2

    def turn(k):
        back = owners - 1 - k
        if owners % 2:
            return (s + back) % owners
        return (near_high + back // 2) % (owners // 2) * 2 + (near_low + back) % 2

    for k in range(owners):
        for j in range(subs):
            chunk_copy(turn(k), j).start()
    barrier = pltpu.get_barrier_semaphore()
    for k in range(1, nb):
        pl.semaphore_signal(barrier, inc=1, device_id={"batch": lax.rem(b + k, nb)},
                            device_id_type=MESH)

    @pl.when(is_owner)
    def _():
        for k in range(n):
            for c in range(pair):
                if k or c:
                    pl.semaphore_signal(
                        barrier, inc=1,
                        device_id={"seq": (s + k) % n, "batch": mate * pair + (side + c) % pair},
                        device_id_type=MESH)

    smalls[0].wait()
    smalls[1].wait()
    head = (gain_v[...] * weight_v[...]).reshape(1, depth)
    high = head.astype(jnp.bfloat16).astype(F32)
    middle = (head - high).astype(jnp.bfloat16).astype(F32)
    low = head - high - middle
    wrow = lax.broadcasted_iota(jnp.int32, (16, depth), 0)
    pieces = jnp.where(wrow == 0, high, jnp.where(wrow == 1, middle, jnp.where(wrow == 2, low, 0.0)))
    pieces = pieces.astype(jnp.bfloat16)

    def part_copy(o):
        return pltpu.make_async_remote_copy(
            part.at[o], rbuf.at[s * pair + side], part_ss, part_rs,
            device_id={"seq": base + o, "batch": lead}, device_id_type=MESH)

    def rw_copy():
        return pltpu.make_async_remote_copy(
            rw_send, rw_recv.at[side * per + half], rw_ss, rw_rs,
            device_id={"seq": rw_at, "batch": lead}, device_id_type=MESH)

    def info_copy(k, i, src, dst):
        return pltpu.make_async_remote_copy(
            src, dst.at[b], info_ss.at[i], info_rs.at[i],
            device_id={"batch": lax.rem(b + k, nb)}, device_id_type=MESH)

    infos = ((len_send, len_recv), (hor_send, hor_recv))
    own_rw = is_owner & (mine == out_o)

    def send_part(o):
        @pl.when(jnp.logical_not(is_owner & (mine == o)))
        def _():
            part_copy(o).start()

    meet = min(1, owners - 1)

    def enter():
        for copy in smalls[2:]:
            copy.wait()
        rw = rew_v[...] * mask_v[...].astype(F32)
        for g in range(gb):
            rw_send[g * R:(g + 1) * R, :] = rw[:, g * LANES:(g + 1) * LANES]
        for r in range(R):
            len_send[r:r + 1, :] = jnp.full((1, LANES), len_s[r], jnp.int32)
            hor_send[r:r + 1, :] = jnp.full((1, LANES), hor_s[r], F32)
        met = jnp.where(is_owner, owners - 1, owners) + nb - 1
        pl.semaphore_wait(barrier, met)
        for before in range(meet):
            send_part(turn(before))

        @pl.when(jnp.logical_not(own_rw))
        def _():
            rw_copy().start()

        for j in range(1, nb):
            for i, (src, dst) in enumerate(infos):
                info_copy(j, i, src, dst).start()

    def squares_of(h):
        squares = jnp.zeros((h.shape[0], LANES), F32)
        for j in range(depth // LANES):
            wide = h[:, j * LANES:(j + 1) * LANES].astype(F32)
            squares = squares + wide * wide
        return squares

    def compute(k, carry):
        o = turn(k)
        for j in range(subs):
            chunk_copy(o, j).wait()
        for g in range(G):
            for r in range(R):
                at = pl.ds(pl.multiple_of(o * L + g * LANES, LANES), LANES)
                h = hv[r, at, :]
                sums = lax.dot_general(pieces, h, (((1,), (1,)), ((), ())),
                                       preferred_element_type=F32)
                row = g * R + r
                part[o, 0, row:row + 1, :] = jnp.sum(sums[0:8], 0, keepdims=True)
                part[o, 1, row:row + 1, :] = jnp.sum(squares_of(h).T, 0, keepdims=True)

        @pl.when(k == meet)
        def _():
            enter()

        @pl.when(k >= meet)
        def _():
            send_part(o)
        return carry

    tiles = depth // TILE

    def unit(r, m):
        return (r * tiles + m) % 2

    def streamed(*accs):
        def acc_of(step, r, m):
            return accs[(step % 2 * R + r) * 2 + unit(r, m)]

        def used(step, r):
            return [accs[(step % 2 * R + r) * 2 + q]
                    for q in sorted({unit(r, m) for m in range(tiles)})]

        for step in range(2):
            for r in range(R):
                for acc in used(step, r):
                    pltpu.matmul_pop(acc)
        for step in range(owners * subs + 1):
            if step < owners * subs:
                o, j = turn(step // subs), step % subs
                chunk_copy(o, j).wait()
                for r in range(R):
                    h = hv[r, pl.ds(pl.multiple_of(o * L + j * S, S), S), :]
                    for m in range(tiles):
                        cols = slice(m * TILE, (m + 1) * TILE)
                        pltpu.matmul_push_rhs(h[:, cols], staging_register=r % 2,
                                              mxu_index=unit(r, m), transpose=True)
                        pltpu.matmul_acc_lhs(acc_of(step, r, m), pieces[:, cols],
                                             load_staged_rhs=r % 2)
                    held_squares[step % 2, r] = squares_of(h)
            if step:
                last = step - 1
                o, j = turn(last // subs), last % subs
                for r in range(R):
                    sums = 0.0
                    for acc in used(last, r):
                        sums = sums + pltpu.matmul_pop(acc)
                    sums = jnp.sum(sums[0:8], 0, keepdims=True)
                    for g in range(S // LANES):
                        row = (j * (S // LANES) + g) * R + r
                        square = held_squares[last % 2, r, g * LANES:(g + 1) * LANES, :]
                        part[o, 0, row:row + 1, :] = sums[:, g * LANES:(g + 1) * LANES]
                        part[o, 1, row:row + 1, :] = jnp.sum(square.T, 0, keepdims=True)
                if j == subs - 1:
                    if last // subs == meet:
                        enter()
                    if last // subs >= meet:
                        send_part(o)

    if depth % TILE == 0 and S == TILE:
        pl.run_scoped(streamed, *[pltpu.ACC(i % 2)((16, TILE), F32) for i in range(4 * R)])
    else:
        lax.fori_loop(0, owners, compute, 0)

    @pl.when(own_rw)
    def _():
        rw_recv[side * per + half] = rw_send[...]

    len_recv[b] = len_send[...]
    hor_recv[b] = hor_send[...]
    for i, (src, dst) in enumerate(infos):
        bytes_of(dst.at[pl.ds(0, nb - 1)], info_rs.at[i]).wait()

    def sum_copy(i, j):
        return pltpu.make_async_remote_copy(
            sum_send, sum_recv.at[mine * pairs + mate], sum_ss, sum_rs,
            device_id={"seq": i, "batch": j}, device_id_type=MESH)

    def each_sum():
        def one(i):
            for j in range(nb):
                never = isinstance(i, int) and not base <= i < base + owners
                if never or j % pair != pair - 1:
                    sum_copy(i, j).start()
                else:
                    @pl.when((i != s) | (j != b))
                    def _():
                        sum_copy(i, j).start()

        if n * nb <= 32:
            for i in range(n):
                one(i)
        else:
            def body(i, carry):
                one(i)
                return carry
            lax.fori_loop(0, n, body, 0)

    def tok_copy(h, j):
        return pltpu.make_async_remote_copy(
            tok_send.at[h * gb + (j * width) // LANES], tok_recv.at[mate], tok_ss, tok_rs,
            device_id={"seq": mine * per + h, "batch": j}, device_id_type=MESH)

    @pl.when(is_owner)
    def _():
        row = lax.broadcasted_iota(jnp.int32, (pair * rows, LANES), 0)
        lane = lax.broadcasted_iota(jnp.int32, (pair * rows, LANES), 1)
        group = row % rows // R
        length = stack([len_recv[mate * pair + c] for c in range(pair) for _ in range(G)])
        reach = stack([hor_recv[mate * pair + c] for c in range(pair) for _ in range(G)])
        rate = -1.0 / reach
        local = group * LANES + lane
        valid = (mine * L + local < length).astype(F32)
        step = 16
        near = [jnp.where(lane < LANES - k, jnp.exp(rate * (k - 1)), 0.0) for k in range(1, step + 1)]
        far = [jnp.where(lane < LANES - k, jnp.exp(rate * k), 0.0) for k in range(step, LANES, step)]
        lead_in = jnp.exp(rate * lane.astype(F32))
        hops = [1 << i for i in range(max(G - 1, 0).bit_length())]
        row_decay = [jnp.where(group + k < G, jnp.exp(rate * (k * LANES)), 0.0) for k in hops]
        into = jnp.where(group < G - 1, jnp.exp(rate * (LANES - 1 - lane).astype(F32)), 0.0)
        power = jnp.exp(rate * (L - 1 - local).astype(F32))
        decay = jnp.exp(rate)
        power_sum = jnp.sum(power, 1, keepdims=True)
        power_squares = jnp.sum(power * power, 1, keepdims=True)
        fixed = jnp.where(lane == 4, power_sum, jnp.where(lane == 5, power_squares, 0.0))

        @pl.when(own_rw)
        def _():
            if pair * per > 1:
                bytes_of(rw_recv.at[pl.ds(0, pair * per - 1)], rw_rs).wait()

        @pl.when(jnp.logical_not(own_rw))
        def _():
            bytes_of(rw_recv, rw_rs).wait()
        gains = stack([rw_recv[c * per + h] for c in range(pair) for h in range(per)])

        rbuf[s * pair + side] = part[mine]
        bytes_of(rbuf.at[pl.ds(0, n * pair - 1)], part_rs).wait()
        projected, squares = [], []
        for c in range(pair):
            first, second = rbuf[c, 0], rbuf[c, 1]
            for k in range(1, n):
                first = first + rbuf[k * pair + c, 0]
                second = second + rbuf[k * pair + c, 1]
            projected.append(first)
            squares.append(second)
        values = stack(projected) * lax.rsqrt(stack(squares) / total + EPS)
        held = values * valid
        change = (gains - values) * valid
        mixed = decay * change + held
        start = jnp.sum(lead_in * mixed, 1, keepdims=True)
        terms = [factor * pltpu.roll(mixed if k < step else held, LANES - k, 1)
                 for k, factor in enumerate(near, 1)]
        while len(terms) > 1:
            terms = [sum(terms[i + 1:i + 2], terms[i]) for i in range(0, len(terms), 2)]
        gae = change + terms[0]
        terms = [factor * pltpu.roll(gae, LANES - k * step, 1) for k, factor in enumerate(far, 1)]
        while len(terms) > 1:
            terms = [sum(terms[i + 1:i + 2], terms[i]) for i in range(0, len(terms), 2)]
        gae = gae + terms[0]
        start = jnp.broadcast_to(start, gae.shape)
        if G > 1:
            for k, factor in zip(hops, row_decay):
                start = start + factor * pltpu.roll(start, pair * rows - k * R, 0)
            gae = gae + into * pltpu.roll(start, pair * rows - R, 0)
        sums = jnp.where(lane == 1, jnp.sum(gae, 1, keepdims=True), fixed)
        sums = jnp.where(lane == 2, 2.0 * jnp.sum(gae * power, 1, keepdims=True), sums)
        sums = jnp.where(lane == 3, jnp.sum(gae * gae, 1, keepdims=True), sums)
        sums = jnp.where((lane == 0) & (group == 0), start, sums)
        for c in range(pair):
            summary = sums[c * rows:c * rows + R]
            for g in range(1, G):
                summary = summary + sums[c * rows + g * R:c * rows + (g + 1) * R]
            sum_send[c * R:(c + 1) * R, :] = summary
        sum_recv[mine * pairs + mate] = sum_send[...]
        each_sum()
        for g in range(G):
            for c in range(pair):
                at = c * rows + g * R
                tok_send[g, 0, c * R:(c + 1) * R, :] = gae[at:at + R]
                tok_send[g, 1, c * R:(c + 1) * R, :] = values[at:at + R]
        for h in range(per):
            for j in range(nb):
                if j % pair != pair - 1:
                    tok_copy(h, j).start()
                else:
                    @pl.when((mine * per + h != s) | (j != b))
                    def _():
                        tok_copy(h, j).start()

                    @pl.when((mine * per + h == s) & (j == b))
                    def _():
                        tok_recv[mate] = tok_send[h * gb + (j * width) // LANES]

    @pl.when(is_owner)
    def _():
        if owners > 1:
            bytes_of(part.at[pl.ds(0, owners - 1)], part_ss).wait()

    @pl.when(jnp.logical_not(is_owner))
    def _():
        bytes_of(part, part_ss).wait()

    @pl.when(jnp.logical_not(own_rw))
    def _():
        rw_copy().wait_send()

    for i, (src, dst) in enumerate(infos):
        bytes_of(dst.at[pl.ds(0, nb - 1)], info_ss.at[i]).wait()

    spots = LANES // width
    spot = b % spots

    def pick(x):
        result = x[:, 0:width]
        for j in range(1, spots):
            result = jnp.where(spot == j, x[:, j * width:(j + 1) * width], result)
        return result

    every = nb * R
    lane = lax.broadcasted_iota(jnp.int32, (every, LANES), 1)
    local = (half * gb + (b * width) // LANES) * LANES + lane
    length = stack([len_recv[c] for c in range(nb)])
    rate = -1.0 / stack([hor_recv[c] for c in range(nb)])
    count = jnp.sum(jnp.minimum(length, T).astype(F32), 0, keepdims=True)
    jump = jnp.exp(rate * float(L))
    power_out = pick(jnp.exp(rate * (L - 1 - local).astype(F32)))
    valid_out = pick((out_o * L + local < length).astype(F32))

    @pl.when(is_owner)
    def _():
        bytes_of(sum_all.at[pl.ds(0, n * nb - 1)], sum_ss).wait()

    @pl.when(own_rw)
    def _():
        bytes_of(tok_all.at[pl.ds(0, per * nb - 1)], tok_ss).wait()

    @pl.when(is_owner & jnp.logical_not(own_rw))
    def _():
        bytes_of(tok_all, tok_ss).wait()

    @pl.when(is_owner)
    def _():
        bytes_of(sum_all.at[pl.ds(0, owners * pairs - 1)], sum_rs).wait()

    @pl.when(jnp.logical_not(is_owner))
    def _():
        bytes_of(sum_recv, sum_rs).wait()

    @pl.when(own_rw)
    def _():
        if pairs > 1:
            bytes_of(tok_recv.at[pl.ds(0, pairs - 1)], tok_rs).wait()

    @pl.when(jnp.logical_not(own_rw))
    def _():
        bytes_of(tok_recv, tok_rs).wait()

    gae = pick(stack([tok_recv[c, 0] for c in range(pairs)]))
    values = pick(stack([tok_recv[c, 1] for c in range(pairs)]))
    acc = jnp.zeros((every, LANES), F32)
    u = jnp.zeros((every, LANES), F32)
    entering = jnp.zeros((every, LANES), F32)
    for o in reversed(range(owners)):
        message = stack([sum_recv[o * pairs + c] for c in range(pairs)])
        factor = jnp.where((lane == 1) | (lane == 3), 1.0,
                           jnp.where((lane == 2) | (lane == 4), u,
                                     jnp.where(lane == 5, u * u, 0.0)))
        acc = acc + message * factor
        entering = jnp.where(out_o == o, u, entering)
        if o:
            u = jnp.broadcast_to(message[:, 0:1], (every, LANES)) + jump * u
    acc = jnp.sum(acc, 0, keepdims=True)
    lane1 = lax.broadcasted_iota(jnp.int32, (1, LANES), 1)
    first = jnp.sum(jnp.where((lane1 == 1) | (lane1 == 4), acc, 0.0), 1, keepdims=True)
    second = jnp.sum(jnp.where((lane1 == 2) | (lane1 == 3) | (lane1 == 5), acc, 0.0), 1, keepdims=True)
    mean = first / count[:, 0:1]
    var = jnp.maximum(second / count[:, 0:1] - mean * mean, 1.0)
    scale = lax.rsqrt(var)
    gae = gae + power_out * entering[:, 0:width]
    out_ref[every:2 * every, :] = (gae + values) * valid_out
    out_ref[0:every, :] = (gae - mean) * valid_out * scale


def per_device(hidden, gain, weight, rewards, mask, lengths, horizon):
    n = lax.axis_size("seq")
    nb = lax.axis_size("batch")
    pair = 2 - nb % 2
    owners = n // 2 if n % 4 == 0 else n
    R, T, depth = hidden.shape
    subs = max(T // owners // TILE, 1)
    block = rewards.shape[1]
    per = n // owners
    G = T // owners // LANES
    gb = block // LANES
    rows = G * R
    Q = pair * R
    pairs = nb // pair
    dma = pltpu.SemaphoreType.DMA
    both = pl.pallas_call(
        functools.partial(kernel, n, nb, pair, owners, subs),
        out_shape=pltpu.VMEM((2 * R * nb, block // nb), F32),
        in_specs=[pl.BlockSpec(memory_space=pl.ANY)] * 7,
        out_specs=pl.BlockSpec(memory_space=pltpu.VMEM),
        scratch_shapes=[
            pltpu.VMEM((R, T, depth), jnp.bfloat16),
            pltpu.VMEM((depth,), F32),
            pltpu.VMEM((depth,), F32),
            pltpu.VMEM((R, block), F32),
            pltpu.VMEM((R, block), jnp.int32),
            pltpu.SMEM((R,), jnp.int32),
            pltpu.SMEM((R,), F32),
            pltpu.VMEM((owners, 2, rows, LANES), F32),
            pltpu.VMEM((n * pair, 2, rows, LANES), F32),
            pltpu.VMEM((gb * R, LANES), F32),
            pltpu.VMEM((pair * per, gb * R, LANES), F32),
            pltpu.VMEM((R, LANES), jnp.int32),
            pltpu.VMEM((nb, R, LANES), jnp.int32),
            pltpu.VMEM((R, LANES), F32),
            pltpu.VMEM((nb, R, LANES), F32),
            pltpu.VMEM((Q, LANES), F32),
            pltpu.VMEM((owners * pairs, Q, LANES), F32),
            pltpu.VMEM((G, 2, Q, LANES), F32),
            pltpu.VMEM((pairs, 2, Q, LANES), F32),
            pltpu.VMEM((n * nb, Q, LANES), F32),
            pltpu.VMEM((per * nb, 2, Q, LANES), F32),
            pltpu.VMEM((2, R, TILE, LANES), F32),
            dma((owners, subs)), dma((6,)),
            dma(()), dma(()),
            dma(()), dma(()),
            dma((2,)), dma((2,)),
            dma(()), dma(()),
            dma(()), dma(()),
        ],
        compiler_params=pltpu.CompilerParams(collective_id=0, has_side_effects=True),
    )(hidden, gain, weight, rewards, mask, lengths, horizon)
    return both[:R * nb], both[R * nb:]


def solution(mesh):
    return jax.shard_map(
        per_device,
        mesh=mesh,
        in_specs=(
            P("batch", None, "seq"),
            P("seq"),
            P("seq"),
            P("batch", "seq"),
            P("batch", "seq"),
            P("batch"),
            P("batch"),
        ),
        out_specs=(P(None, ("seq", "batch")), P(None, ("seq", "batch"))),
        check_vma=False,
    )
```

```python
import functools

import jax
import jax.numpy as jnp
from jax import lax
from jax.experimental import pallas as pl
from jax.experimental.pallas import tpu as pltpu
from jax.sharding import PartitionSpec as P

EPS = 1e-05
LANES = 128
TILE = 256
F32 = jnp.float32
MESH = pl.DeviceIdType.MESH


def bytes_of(ref, sem):
    return pltpu.make_async_copy(ref, ref, sem)


def stack(pieces):
    return pieces[0] if len(pieces) == 1 else jnp.concatenate(pieces, 0)


def kernel(n, nb, pair, owners, subs, stream, hidden, gain, weight, rewards, mask, lengths, horizon,
           out_ref,
           hv, gain_v, weight_v, rew_v, mask_v, len_s, hor_s,
           part, rbuf, rw_send, rw_recv, len_send, len_recv, hor_send, hor_recv,
           sum_send, sum_recv, tok_send, tok_recv, both_v, both_m, any_rows, held_squares,
           chunk_sem, small_sem, sent, early, part_rs, late):
    R, T, depth = hidden.shape
    block = rewards.shape[1]
    width = block // nb
    per = n // owners
    base = (n - owners) // 2
    L = T // owners
    G = L // LANES
    gb = block // LANES
    rows = G * R
    Q = pair * R
    pairs = nb // pair
    total = depth * n
    s = lax.axis_index("seq")
    b = lax.axis_index("batch")
    side = b % pair
    mate = b // pair
    lead = mate * pair + pair - 1
    is_owner = (s >= base) & (s < base + owners) & (side == pair - 1)
    mine = s - base
    out_o = s // per
    half = s % per
    rw_at = base + out_o

    S = L // subs
    srows = rows // subs
    near_high = s * (owners // 2) // n
    near_low = s % 2

    def turn(k):
        back = owners - 1 - k
        if owners % 2:
            return (s + back) % owners
        return (near_high + back // 2) % (owners // 2) * 2 + (near_low + back) % 2

    def chunk_copy(c):
        span = pl.ds(turn(c // subs) * L + c % subs * S, S)
        return pltpu.make_async_copy(hidden.at[:, span, :], hv.at[:, span, :], chunk_sem.at[c])

    def wait_rows(count, sem):
        if count:
            bytes_of(any_rows.at[pl.ds(0, count)], sem).wait()

    pltpu.make_async_copy(gain, gain_v, small_sem.at[0]).start()
    pltpu.make_async_copy(weight, weight_v, small_sem.at[0]).start()
    for c in range(owners * subs):
        chunk_copy(c).start()
    pltpu.make_async_copy(rewards, rew_v, small_sem.at[1]).start()
    pltpu.make_async_copy(mask, mask_v, small_sem.at[1]).start()
    ends = [pltpu.make_async_copy(lengths, len_s, small_sem.at[2]),
            pltpu.make_async_copy(horizon, hor_s, small_sem.at[3])]
    for copy in ends:
        copy.start()
    barrier = pltpu.get_barrier_semaphore()
    for k in range(1, nb):
        pl.semaphore_signal(barrier, inc=1, device_id={"batch": lax.rem(b + k, nb)},
                            device_id_type=MESH)

    @pl.when(is_owner)
    def _():
        for k in range(n):
            for c in range(pair):
                if k or c:
                    pl.semaphore_signal(
                        barrier, inc=1,
                        device_id={"seq": (s + k) % n, "batch": mate * pair + (side + c) % pair},
                        device_id_type=MESH)

    def head_pieces():
        bytes_of(both_v.at[pl.ds(0, 2 * depth)], small_sem.at[0]).wait()
        head = (gain_v[...] * weight_v[...]).reshape(1, depth)
        high = head.astype(jnp.bfloat16).astype(F32)
        middle = (head - high).astype(jnp.bfloat16).astype(F32)
        low = head - high - middle
        wrow = lax.broadcasted_iota(jnp.int32, (16, depth), 0)
        pieces = jnp.where(wrow == 0, high, jnp.where(wrow == 1, middle, jnp.where(wrow == 2, low, 0.0)))
        return pieces.astype(jnp.bfloat16)

    def part_copy(o, j):
        return pltpu.make_async_remote_copy(
            part.at[o, j], rbuf.at[s * pair + side, j], sent, part_rs,
            device_id={"seq": base + o, "batch": lead}, device_id_type=MESH)

    def rw_copy():
        return pltpu.make_async_remote_copy(
            rw_send, rw_recv.at[side * per + half], sent, early,
            device_id={"seq": rw_at, "batch": lead}, device_id_type=MESH)

    def info_copy(k, src, dst):
        return pltpu.make_async_remote_copy(
            src, dst.at[b], sent, early,
            device_id={"batch": lax.rem(b + k, nb)}, device_id_type=MESH)

    infos = ((len_send, len_recv), (hor_send, hor_recv))
    own_rw = is_owner & (mine == out_o)

    def send_part(o, j):
        @pl.when(jnp.logical_not(is_owner & (mine == o)))
        def _():
            part_copy(o, j).start()

    meet = min(2, owners * subs - 1)

    def enter():
        bytes_of(both_m, small_sem.at[1]).wait()
        for copy in ends:
            copy.wait()
        rw = rew_v[...] * mask_v[...].astype(F32)
        for g in range(gb):
            rw_send[g * R:(g + 1) * R, :] = rw[:, g * LANES:(g + 1) * LANES]
        for r in range(R):
            len_send[r:r + 1, :] = jnp.full((1, LANES), len_s[r], jnp.int32)
            hor_send[r:r + 1, :] = jnp.full((1, LANES), hor_s[r], F32)
        met = jnp.where(is_owner, owners - 1, owners) + nb - 1
        pl.semaphore_wait(barrier, met)

        @pl.when(jnp.logical_not(own_rw))
        def _():
            rw_copy().start()

        for j in range(1, nb):
            for src, dst in infos:
                info_copy(j, src, dst).start()

    def squares_of(h):
        squares = jnp.zeros((h.shape[0], LANES), F32)
        for j in range(depth // LANES):
            wide = h[:, j * LANES:(j + 1) * LANES].astype(F32)
            squares = squares + wide * wide
        return squares

    def compute(k, pieces):
        o = turn(k)
        for j in range(subs):
            chunk_copy(k * subs + j).wait()
        for g in range(G):
            for r in range(R):
                at = pl.ds(pl.multiple_of(o * L + g * LANES, LANES), LANES)
                h = hv[r, at, :]
                sums = lax.dot_general(pieces, h, (((1,), (1,)), ((), ())),
                                       preferred_element_type=F32)
                j, row = divmod(g * R + r, srows)
                part[o, j, 0, row:row + 1, :] = jnp.sum(sums[0:8], 0, keepdims=True)
                part[o, j, 1, row:row + 1, :] = jnp.sum(squares_of(h).T, 0, keepdims=True)

        @pl.when(k == 0)
        def _():
            enter()

        for j in range(subs):
            send_part(o, j)
        return pieces

    def streamed(*accs):
        for acc in accs:
            pltpu.matmul_pop(acc)
        pieces = None
        units = [(r, m) for r in range(R) for m in range(2)]
        for step in range(owners * subs + 1):
            if step < owners * subs:
                o, j = turn(step // subs), step % subs
                chunk_copy(step).wait()
                blocks = [hv[r, pl.ds(pl.multiple_of(o * L + j * S, S), S), :] for r in range(R)]
                if step == 0:
                    for r, m in units:
                        pltpu.matmul_push_rhs(blocks[r][:, m * TILE:(m + 1) * TILE],
                                              staging_register=r, mxu_index=m, transpose=True)
                    for r in range(R):
                        held_squares[step % 2, r] = squares_of(blocks[r])
                    pieces = head_pieces()
                for r, m in units:
                    if step:
                        pltpu.matmul_push_rhs(blocks[r][:, m * TILE:(m + 1) * TILE],
                                              staging_register=r, mxu_index=m, transpose=True)
                    pltpu.matmul_acc_lhs(accs[(step % 2 * R + r) * 2 + m],
                                         pieces[:, m * TILE:(m + 1) * TILE], load_staged_rhs=r)
                if step:
                    for r in range(R):
                        held_squares[step % 2, r] = squares_of(blocks[r])
            if step:
                last = step - 1
                o, j = turn(last // subs), last % subs
                for r in range(R):
                    at = (last % 2 * R + r) * 2
                    sums = pltpu.matmul_pop(accs[at]) + pltpu.matmul_pop(accs[at + 1])
                    sums = jnp.sum(sums[0:8], 0, keepdims=True)
                    for g in range(S // LANES):
                        row = g * R + r
                        square = held_squares[last % 2, r, g * LANES:(g + 1) * LANES, :]
                        part[o, j, 0, row:row + 1, :] = sums[:, g * LANES:(g + 1) * LANES]
                        part[o, j, 1, row:row + 1, :] = jnp.sum(square.T, 0, keepdims=True)
                if last == meet:
                    enter()
                for c in range(last if last > meet else 0, last + 1 if last >= meet else 0):
                    send_part(turn(c // subs), c % subs)

    if stream:
        pl.run_scoped(streamed, *[pltpu.ACC(i % 2)((16, TILE), F32) for i in range(4 * R)])
    else:
        lax.fori_loop(0, owners, compute, head_pieces())

    @pl.when(own_rw)
    def _():
        rw_recv[side * per + half] = rw_send[...]

    len_recv[b] = len_send[...]
    hor_recv[b] = hor_send[...]
    info_rows = 2 * R * (nb - 1)

    @pl.when(jnp.logical_not(is_owner))
    def _():
        wait_rows(info_rows, early)

    @pl.when(own_rw)
    def _():
        wait_rows(info_rows + gb * R * (pair * per - 1), early)

    @pl.when(is_owner & jnp.logical_not(own_rw))
    def _():
        wait_rows(info_rows + gb * R * pair * per, early)

    def sum_copy(i, j):
        return pltpu.make_async_remote_copy(
            sum_send, sum_recv.at[mine * pairs + mate], sent, late,
            device_id={"seq": i, "batch": j}, device_id_type=MESH)

    def each_sum():
        def one(i):
            for j in range(nb):
                never = isinstance(i, int) and not base <= i < base + owners
                if never or j % pair != pair - 1:
                    sum_copy(i, j).start()
                else:
                    @pl.when((i != s) | (j != b))
                    def _():
                        sum_copy(i, j).start()

        if n * nb <= 32:
            for i in range(n):
                one(i)
        else:
            def body(i, carry):
                one(i)
                return carry
            lax.fori_loop(0, n, body, 0)

    def tok_copy(h, j):
        return pltpu.make_async_remote_copy(
            tok_send.at[h * gb + (j * width) // LANES], tok_recv.at[mate], sent, late,
            device_id={"seq": mine * per + h, "batch": j}, device_id_type=MESH)

    @pl.when(is_owner)
    def _():
        row = lax.broadcasted_iota(jnp.int32, (pair * rows, LANES), 0)
        lane = lax.broadcasted_iota(jnp.int32, (pair * rows, LANES), 1)
        group = row % rows // R
        length = stack([len_recv[mate * pair + c] for c in range(pair) for _ in range(G)])
        reach = stack([hor_recv[mate * pair + c] for c in range(pair) for _ in range(G)])
        rate = -1.0 / reach
        local = group * LANES + lane
        valid = (mine * L + local < length).astype(F32)
        step = 16
        near = [jnp.where(lane < LANES - k, jnp.exp(rate * (k - 1)), 0.0) for k in range(1, step + 1)]
        far = [jnp.where(lane < LANES - k, jnp.exp(rate * k), 0.0) for k in range(step, LANES, step)]
        lead_in = jnp.exp(rate * lane.astype(F32))
        hops = [1 << i for i in range(max(G - 1, 0).bit_length())]
        row_decay = [jnp.where(group + k < G, jnp.exp(rate * (k * LANES)), 0.0) for k in hops]
        into = jnp.where(group < G - 1, jnp.exp(rate * (LANES - 1 - lane).astype(F32)), 0.0)
        power = jnp.exp(rate * (L - 1 - local).astype(F32))
        decay = jnp.exp(rate)
        gains = stack([rw_recv[c * per + h] for c in range(pair) for h in range(per)])

        rbuf[s * pair + side] = part[mine]
        bytes_of(rbuf.at[pl.ds(0, n * pair - 1)], part_rs).wait()
        projected, squares = [], []
        for c in range(pair):
            for j in range(subs):
                first, second = rbuf[c, j, 0], rbuf[c, j, 1]
                for k in range(1, n):
                    first = first + rbuf[k * pair + c, j, 0]
                    second = second + rbuf[k * pair + c, j, 1]
                projected.append(first)
                squares.append(second)
        values = stack(projected) * lax.rsqrt(stack(squares) / total + EPS)
        held = values * valid
        change = (gains - values) * valid
        mixed = decay * change + held
        start = jnp.sum(lead_in * mixed, 1, keepdims=True)
        terms = [factor * pltpu.roll(mixed if k < step else held, LANES - k, 1)
                 for k, factor in enumerate(near, 1)]
        while len(terms) > 1:
            terms = [sum(terms[i + 1:i + 2], terms[i]) for i in range(0, len(terms), 2)]
        gae = change + terms[0]
        terms = [factor * pltpu.roll(gae, LANES - k * step, 1) for k, factor in enumerate(far, 1)]
        while len(terms) > 1:
            terms = [sum(terms[i + 1:i + 2], terms[i]) for i in range(0, len(terms), 2)]
        gae = gae + terms[0]
        start = jnp.broadcast_to(start, gae.shape)
        if G > 1:
            for k, factor in zip(hops, row_decay):
                start = start + factor * pltpu.roll(start, pair * rows - k * R, 0)
            gae = gae + into * pltpu.roll(start, pair * rows - R, 0)
        sums = jnp.where(lane == 1, jnp.sum(gae, 1, keepdims=True), 0.0)
        sums = jnp.where(lane == 2, 2.0 * jnp.sum(gae * power, 1, keepdims=True), sums)
        sums = jnp.where(lane == 3, jnp.sum(gae * gae, 1, keepdims=True), sums)
        sums = jnp.where((lane == 0) & (group == 0), start, sums)
        if G & (G - 1) == 0:
            for k in hops:
                sums = sums + pltpu.roll(sums, pair * rows - k * R, 0)
            for c in range(pair):
                sum_send[c * R:(c + 1) * R, :] = sums[c * rows:c * rows + R]
        else:
            for c in range(pair):
                summary = sums[c * rows:c * rows + R]
                for g in range(1, G):
                    summary = summary + sums[c * rows + g * R:c * rows + (g + 1) * R]
                sum_send[c * R:(c + 1) * R, :] = summary
        sum_recv[mine * pairs + mate] = sum_send[...]
        each_sum()
        for g in range(G):
            for c in range(pair):
                at = c * rows + g * R
                tok_send[g, 0, c * R:(c + 1) * R, :] = gae[at:at + R]
                tok_send[g, 1, c * R:(c + 1) * R, :] = values[at:at + R]
        for h in range(per):
            for j in range(nb):
                if j % pair != pair - 1:
                    tok_copy(h, j).start()
                else:
                    @pl.when((mine * per + h != s) | (j != b))
                    def _():
                        tok_copy(h, j).start()

                    @pl.when((mine * per + h == s) & (j == b))
                    def _():
                        tok_recv[mate] = tok_send[h * gb + (j * width) // LANES]

    spots = LANES // width
    spot = b % spots

    def pick(x):
        result = x[:, 0:width]
        for j in range(1, spots):
            result = jnp.where(spot == j, x[:, j * width:(j + 1) * width], result)
        return result

    every = nb * R
    lane = lax.broadcasted_iota(jnp.int32, (every, LANES), 1)
    local = (half * gb + (b * width) // LANES) * LANES + lane
    length = stack([len_recv[c] for c in range(nb)])
    rate = -1.0 / stack([hor_recv[c] for c in range(nb)])
    count = jnp.sum(jnp.minimum(length, T).astype(F32), 0, keepdims=True)
    share = 1.0 / count
    jump = jnp.exp(rate * float(L))
    power_out = pick(jnp.exp(rate * (L - 1 - local).astype(F32)))
    valid_out = pick((out_o * L + local < length).astype(F32))
    power = [jnp.exp(rate * (L - 1 - g * LANES - lane).astype(F32)) for g in range(G)]
    power_sum = jnp.broadcast_to(jnp.sum(sum(power[1:], power[0]), 1, keepdims=True), (every, LANES))
    power = [x * x for x in power]
    power_squares = jnp.broadcast_to(jnp.sum(sum(power[1:], power[0]), 1, keepdims=True), (every, LANES))

    part_rows = 2 * rows * (owners - 1) + info_rows
    sum_rows = Q * owners * pairs
    tok_rows = 2 * Q * pairs

    @pl.when(jnp.logical_not(is_owner))
    def _():
        wait_rows(part_rows + 2 * rows + gb * R, sent)
        wait_rows(sum_rows + tok_rows, late)

    @pl.when(own_rw)
    def _():
        wait_rows(part_rows + Q * (n * nb - 1) + 2 * Q * (per * nb - 1), sent)
        wait_rows(sum_rows - Q + tok_rows - 2 * Q, late)

    @pl.when(is_owner & jnp.logical_not(own_rw))
    def _():
        wait_rows(part_rows + gb * R + Q * (n * nb - 1) + 2 * Q * per * nb, sent)
        wait_rows(sum_rows - Q + tok_rows, late)

    gae = pick(stack([tok_recv[c, 0] for c in range(pairs)]))
    values = pick(stack([tok_recv[c, 1] for c in range(pairs)]))
    messages = [stack([sum_recv[o * pairs + c] for c in range(pairs)]) for o in range(owners)]

    def spread(o, i):
        return jnp.broadcast_to(messages[o][:, i:i + 1], (every, LANES))

    u = spread(owners - 1, 0)
    first = sum([spread(o, 1) for o in range(1, owners)], spread(0, 1))
    second = sum([spread(o, 3) for o in range(1, owners)], spread(0, 3))
    entering = jnp.zeros((every, LANES), F32)
    for o in reversed(range(owners - 1)):
        first = first + u * power_sum
        second = second + u * (spread(o, 2) + u * power_squares)
        entering = jnp.where(out_o == o, u, entering)
        if o:
            u = spread(o, 0) + jump * u
    mean = jnp.sum(first, 0, keepdims=True) * share
    var = jnp.maximum(jnp.sum(second, 0, keepdims=True) * share - mean * mean, 1.0)
    scale = lax.rsqrt(var)
    gae = gae + power_out * entering[:, 0:width]
    out_ref[every:2 * every, :] = (gae + values) * valid_out
    out_ref[0:every, :] = (gae - mean[:, 0:width]) * valid_out * scale[:, 0:width]


def per_device(hidden, gain, weight, rewards, mask, lengths, horizon):
    n = lax.axis_size("seq")
    nb = lax.axis_size("batch")
    pair = 2 - nb % 2
    owners = n // 2 if n % 4 == 0 else n
    R, T, depth = hidden.shape
    subs = max(T // owners // TILE, 1)
    chunks = owners * subs
    stream = R == 2 and depth == 2 * TILE and T == chunks * TILE
    block = rewards.shape[1]
    per = n // owners
    G = T // owners // LANES
    gb = block // LANES
    rows = G * R
    Q = pair * R
    pairs = nb // pair
    dma = pltpu.SemaphoreType.DMA
    both = pl.pallas_call(
        functools.partial(kernel, n, nb, pair, owners, subs, stream),
        out_shape=pltpu.VMEM((2 * R * nb, block // nb), F32),
        in_specs=[pl.BlockSpec(memory_space=pl.ANY)] * 7,
        out_specs=pl.BlockSpec(memory_space=pltpu.VMEM),
        scratch_shapes=[
            pltpu.VMEM((R, T, depth), jnp.bfloat16),
            pltpu.VMEM((depth,), F32),
            pltpu.VMEM((depth,), F32),
            pltpu.VMEM((R, block), F32),
            pltpu.VMEM((R, block), jnp.int32),
            pltpu.SMEM((R,), jnp.int32),
            pltpu.SMEM((R,), F32),
            pltpu.VMEM((owners, subs, 2, rows // subs, LANES), F32),
            pltpu.VMEM((n * pair, subs, 2, rows // subs, LANES), F32),
            pltpu.VMEM((gb * R, LANES), F32),
            pltpu.VMEM((pair * per, gb * R, LANES), F32),
            pltpu.VMEM((R, LANES), jnp.int32),
            pltpu.VMEM((nb, R, LANES), jnp.int32),
            pltpu.VMEM((R, LANES), F32),
            pltpu.VMEM((nb, R, LANES), F32),
            pltpu.VMEM((Q, LANES), F32),
            pltpu.VMEM((owners * pairs, Q, LANES), F32),
            pltpu.VMEM((G, 2, Q, LANES), F32),
            pltpu.VMEM((pairs, 2, Q, LANES), F32),
            pltpu.VMEM((2 * depth,), F32),
            pltpu.VMEM((2 * R, block), F32),
            pltpu.VMEM((2 * owners * rows + 2 * R * nb + Q * n * nb + 2 * Q * per * nb + rows, LANES), F32),
            pltpu.VMEM((2, R, TILE, LANES), F32),
            dma((chunks,)), dma((4,)), dma(()), dma(()), dma(()), dma(()),
        ],
        compiler_params=pltpu.CompilerParams(collective_id=0, has_side_effects=True),
    )(hidden, gain, weight, rewards, mask, lengths, horizon)
    return both[:R * nb], both[R * nb:]


def solution(mesh):
    return jax.shard_map(
        per_device,
        mesh=mesh,
        in_specs=(
            P("batch", None, "seq"),
            P("seq"),
            P("seq"),
            P("batch", "seq"),
            P("batch", "seq"),
            P("batch"),
            P("batch"),
        ),
        out_specs=(P(None, ("seq", "batch")), P(None, ("seq", "batch"))),
        check_vma=False,
    )
```

```python
import functools

import jax
import jax.numpy as jnp
from jax import lax
from jax.experimental import pallas as pl
from jax.experimental.pallas import tpu as pltpu
from jax.sharding import PartitionSpec as P

EPS = 1e-05
LANES = 128
TILE = 256
F32 = jnp.float32
MESH = pl.DeviceIdType.MESH


def bytes_of(ref, sem):
    return pltpu.make_async_copy(ref, ref, sem)


def stack(pieces):
    return pieces[0] if len(pieces) == 1 else jnp.concatenate(pieces, 0)


def kernel(n, nb, pair, owners, subs, stream, hidden, gain, weight, rewards, mask, lengths, horizon,
           out_ref,
           hv, gain_v, weight_v, rew_v, mask_v, len_s, hor_s,
           part, rbuf, rw_send, rw_recv, len_send, len_recv, hor_send, hor_recv,
           sum_send, sum_recv, tok_send, tok_recv, both_v, both_m, any_rows, held_squares,
           chunk_sem, small_sem, sent, early, part_rs, late):
    R, T, depth = hidden.shape
    block = rewards.shape[1]
    width = block // nb
    per = n // owners
    base = (n - owners) // 2
    L = T // owners
    G = L // LANES
    gb = block // LANES
    rows = G * R
    Q = pair * R
    pairs = nb // pair
    total = depth * n
    s = lax.axis_index("seq")
    b = lax.axis_index("batch")
    side = b % pair
    mate = b // pair
    lead = mate * pair + pair - 1
    is_owner = (s >= base) & (s < base + owners) & (side == pair - 1)
    mine = s - base
    out_o = s // per
    half = s % per
    rw_at = base + out_o

    S = L // subs
    srows = rows // subs
    near_high = s * (owners // 2) // n
    near_low = s % 2

    def turn(k):
        back = owners - 1 - k
        if owners % 2:
            return (s + back) % owners
        return (near_high + back // 2) % (owners // 2) * 2 + (near_low + back) % 2

    plan = [(c, tuple(range(R))) for c in range(owners * subs)]

    def chunk_copy(c, rs, i):
        span = pl.ds(turn(c // subs) * L + c % subs * S, S)
        at = slice(None) if len(rs) == R else rs[0]
        return pltpu.make_async_copy(hidden.at[at, span, :], hv.at[at, span, :], chunk_sem.at[i])

    def wait_rows(count, sem):
        if count:
            bytes_of(any_rows.at[pl.ds(0, count)], sem).wait()

    smalls = [
        pltpu.make_async_copy(src, dst, small_sem.at[i])
        for i, src, dst in ((0, gain, gain_v), (0, weight, weight_v), (1, rewards, rew_v),
                            (1, mask, mask_v), (2, lengths, len_s), (3, horizon, hor_s))]
    for i, (c, rs) in enumerate(plan):
        chunk_copy(c, rs, i).start(priority=int(i > 1))
        if i == 0:
            for copy in smalls:
                copy.start()
    barrier = pltpu.get_barrier_semaphore()
    for k in range(1, nb):
        pl.semaphore_signal(barrier, inc=1, device_id={"batch": lax.rem(b + k, nb)},
                            device_id_type=MESH)

    @pl.when(is_owner)
    def _():
        for k in range(n):
            for c in range(pair):
                if k or c:
                    pl.semaphore_signal(
                        barrier, inc=1,
                        device_id={"seq": (s + k) % n, "batch": mate * pair + (side + c) % pair},
                        device_id_type=MESH)

    def head_pieces():
        bytes_of(both_v.at[pl.ds(0, 2 * depth)], small_sem.at[0]).wait()
        head = (gain_v[...] * weight_v[...]).reshape(1, depth)
        high = head.astype(jnp.bfloat16).astype(F32)
        middle = (head - high).astype(jnp.bfloat16).astype(F32)
        low = head - high - middle
        wrow = lax.broadcasted_iota(jnp.int32, (16, depth), 0)
        pieces = jnp.where(wrow == 0, high, jnp.where(wrow == 1, middle, jnp.where(wrow == 2, low, 0.0)))
        return pieces.astype(jnp.bfloat16)

    def part_copy(o, j):
        return pltpu.make_async_remote_copy(
            part.at[o, j], rbuf.at[s * pair + side, j], sent, part_rs,
            device_id={"seq": base + o, "batch": lead}, device_id_type=MESH)

    def rw_copy():
        return pltpu.make_async_remote_copy(
            rw_send, rw_recv.at[side * per + half], sent, early,
            device_id={"seq": rw_at, "batch": lead}, device_id_type=MESH)

    def info_copy(k, src, dst):
        return pltpu.make_async_remote_copy(
            src, dst.at[b], sent, early,
            device_id={"batch": lax.rem(b + k, nb)}, device_id_type=MESH)

    infos = ((len_send, len_recv), (hor_send, hor_recv))
    own_rw = is_owner & (mine == out_o)

    def send_part(o, j):
        @pl.when(jnp.logical_not(is_owner & (mine == o)))
        def _():
            part_copy(o, j).start()

    meet = min(1, owners * subs - 1)

    pieces = head_pieces()
    bytes_of(both_m, small_sem.at[1]).wait()
    for copy in smalls[4:]:
        copy.wait()
    rw = rew_v[...] * mask_v[...].astype(F32)
    for g in range(gb):
        rw_send[g * R:(g + 1) * R, :] = rw[:, g * LANES:(g + 1) * LANES]
    for r in range(R):
        len_send[r:r + 1, :] = jnp.full((1, LANES), len_s[r], jnp.int32)
        hor_send[r:r + 1, :] = jnp.full((1, LANES), hor_s[r], F32)

    def enter():
        met = jnp.where(is_owner, owners - 1, owners) + nb - 1
        pl.semaphore_wait(barrier, met)

        @pl.when(jnp.logical_not(own_rw))
        def _():
            rw_copy().start()

        for j in range(1, nb):
            for src, dst in infos:
                info_copy(j, src, dst).start()

    def squares_of(h):
        squares = jnp.zeros((h.shape[0], LANES), F32)
        for j in range(depth // LANES):
            wide = h[:, j * LANES:(j + 1) * LANES].astype(F32)
            squares = squares + wide * wide
        return squares

    def compute(k, carry):
        o = turn(k)
        for j in range(subs):
            chunk_copy(k * subs + j, range(R), k * subs + j).wait()
        for g in range(G):
            for r in range(R):
                at = pl.ds(pl.multiple_of(o * L + g * LANES, LANES), LANES)
                h = hv[r, at, :]
                sums = lax.dot_general(pieces, h, (((1,), (1,)), ((), ())),
                                       preferred_element_type=F32)
                j, row = divmod(g * R + r, srows)
                part[o, j, 0, row:row + 1, :] = jnp.sum(sums[0:8], 0, keepdims=True)
                part[o, j, 1, row:row + 1, :] = jnp.sum(squares_of(h).T, 0, keepdims=True)

        @pl.when(k == 0)
        def _():
            enter()

        for j in range(subs):
            send_part(o, j)
        return carry

    def streamed(*accs):
        for acc in accs:
            pltpu.matmul_pop(acc)
        for step in range(len(plan) + 1):
            if step < len(plan):
                c, rs = plan[step]
                o, j = turn(c // subs), c % subs
                chunk_copy(c, rs, step).wait()
                for r in rs:
                    h = hv[r, pl.ds(pl.multiple_of(o * L + j * S, S), S), :]
                    for m in range(2):
                        cols = slice(m * TILE, (m + 1) * TILE)
                        pltpu.matmul_push_rhs(h[:, cols], staging_register=r, mxu_index=m,
                                              transpose=True)
                        pltpu.matmul_acc_lhs(accs[(step % 2 * R + r) * 2 + m], pieces[:, cols],
                                             load_staged_rhs=r)
                    held_squares[step % 2, r] = squares_of(h)
            if step:
                last = step - 1
                c, rs = plan[last]
                o, j = turn(c // subs), c % subs
                for r in rs:
                    at = (last % 2 * R + r) * 2
                    sums = pltpu.matmul_pop(accs[at]) + pltpu.matmul_pop(accs[at + 1])
                    sums = jnp.sum(sums[0:8], 0, keepdims=True)
                    for g in range(S // LANES):
                        row = g * R + r
                        square = held_squares[last % 2, r, g * LANES:(g + 1) * LANES, :]
                        part[o, j, 0, row:row + 1, :] = sums[:, g * LANES:(g + 1) * LANES]
                        part[o, j, 1, row:row + 1, :] = jnp.sum(square.T, 0, keepdims=True)
                if last == meet:
                    enter()
                    for i in range(c):
                        send_part(turn(i // subs), i % subs)
                if last >= meet and rs[-1] == R - 1:
                    send_part(o, j)

    if stream:
        pl.run_scoped(streamed, *[pltpu.ACC(i % 2)((16, TILE), F32) for i in range(4 * R)])
    else:
        lax.fori_loop(0, owners, compute, 0)

    @pl.when(own_rw)
    def _():
        rw_recv[side * per + half] = rw_send[...]

    len_recv[b] = len_send[...]
    hor_recv[b] = hor_send[...]
    info_rows = 2 * R * (nb - 1)

    @pl.when(jnp.logical_not(is_owner))
    def _():
        wait_rows(info_rows, early)

    @pl.when(own_rw)
    def _():
        wait_rows(info_rows + gb * R * (pair * per - 1), early)

    @pl.when(is_owner & jnp.logical_not(own_rw))
    def _():
        wait_rows(info_rows + gb * R * pair * per, early)

    def sum_copy(i, j):
        return pltpu.make_async_remote_copy(
            sum_send, sum_recv.at[mine * pairs + mate], sent, late,
            device_id={"seq": i, "batch": j}, device_id_type=MESH)

    def each_sum():
        def one(i):
            for j in range(nb):
                never = isinstance(i, int) and not base <= i < base + owners
                if never or j % pair != pair - 1:
                    sum_copy(i, j).start()
                else:
                    @pl.when((i != s) | (j != b))
                    def _():
                        sum_copy(i, j).start()

        if n * nb <= 32:
            for i in range(n):
                one(i)
        else:
            def body(i, carry):
                one(i)
                return carry
            lax.fori_loop(0, n, body, 0)

    def tok_copy(h, j):
        return pltpu.make_async_remote_copy(
            tok_send.at[h * gb + (j * width) // LANES], tok_recv.at[mate], sent, late,
            device_id={"seq": mine * per + h, "batch": j}, device_id_type=MESH)

    @pl.when(is_owner)
    def _():
        row = lax.broadcasted_iota(jnp.int32, (pair * rows, LANES), 0)
        lane = lax.broadcasted_iota(jnp.int32, (pair * rows, LANES), 1)
        group = row % rows // R
        length = stack([len_recv[mate * pair + c] for c in range(pair) for _ in range(G)])
        reach = stack([hor_recv[mate * pair + c] for c in range(pair) for _ in range(G)])
        rate = -1.0 / reach
        local = group * LANES + lane
        valid = (mine * L + local < length).astype(F32)
        step = 16
        near = [jnp.where(lane < LANES - k, jnp.exp(rate * (k - 1)), 0.0) for k in range(1, step + 1)]
        far = [jnp.where(lane < LANES - k, jnp.exp(rate * k), 0.0) for k in range(step, LANES, step)]
        lead_in = jnp.exp(rate * lane.astype(F32))
        hops = [1 << i for i in range(max(G - 1, 0).bit_length())]
        row_decay = [jnp.where(group + k < G, jnp.exp(rate * (k * LANES)), 0.0) for k in hops]
        into = jnp.where(group < G - 1, jnp.exp(rate * (LANES - 1 - lane).astype(F32)), 0.0)
        power = jnp.exp(rate * (L - 1 - local).astype(F32))
        decay = jnp.exp(rate)
        gains = stack([rw_recv[c * per + h] for c in range(pair) for h in range(per)])

        rbuf[s * pair + side] = part[mine]
        bytes_of(rbuf.at[pl.ds(0, n * pair - 1)], part_rs).wait()
        projected, squares = [], []
        for c in range(pair):
            for j in range(subs):
                first, second = rbuf[c, j, 0], rbuf[c, j, 1]
                for k in range(1, n):
                    first = first + rbuf[k * pair + c, j, 0]
                    second = second + rbuf[k * pair + c, j, 1]
                projected.append(first)
                squares.append(second)
        values = stack(projected) * lax.rsqrt(stack(squares) / total + EPS)
        held = values * valid
        change = (gains - values) * valid
        mixed = decay * change + held
        start = jnp.sum(lead_in * mixed, 1, keepdims=True)
        terms = [factor * pltpu.roll(mixed if k < step else held, LANES - k, 1)
                 for k, factor in enumerate(near, 1)]
        while len(terms) > 1:
            terms = [sum(terms[i + 1:i + 2], terms[i]) for i in range(0, len(terms), 2)]
        gae = change + terms[0]
        terms = [factor * pltpu.roll(gae, LANES - k * step, 1) for k, factor in enumerate(far, 1)]
        while len(terms) > 1:
            terms = [sum(terms[i + 1:i + 2], terms[i]) for i in range(0, len(terms), 2)]
        gae = gae + terms[0]
        start = jnp.broadcast_to(start, gae.shape)
        if G > 1:
            for k, factor in zip(hops, row_decay):
                start = start + factor * pltpu.roll(start, pair * rows - k * R, 0)
            gae = gae + into * pltpu.roll(start, pair * rows - R, 0)
        sums = jnp.where(lane == 1, jnp.sum(gae, 1, keepdims=True), 0.0)
        sums = jnp.where(lane == 2, 2.0 * jnp.sum(gae * power, 1, keepdims=True), sums)
        sums = jnp.where(lane == 3, jnp.sum(gae * gae, 1, keepdims=True), sums)
        sums = jnp.where((lane == 0) & (group == 0), start, sums)
        if G & (G - 1) == 0:
            for k in hops:
                sums = sums + pltpu.roll(sums, pair * rows - k * R, 0)
            for c in range(pair):
                sum_send[c * R:(c + 1) * R, :] = sums[c * rows:c * rows + R]
        else:
            for c in range(pair):
                summary = sums[c * rows:c * rows + R]
                for g in range(1, G):
                    summary = summary + sums[c * rows + g * R:c * rows + (g + 1) * R]
                sum_send[c * R:(c + 1) * R, :] = summary
        sum_recv[mine * pairs + mate] = sum_send[...]
        each_sum()
        for g in range(G):
            for c in range(pair):
                at = c * rows + g * R
                tok_send[g, 0, c * R:(c + 1) * R, :] = gae[at:at + R]
                tok_send[g, 1, c * R:(c + 1) * R, :] = values[at:at + R]
        for h in range(per):
            for j in range(nb):
                if j % pair != pair - 1:
                    tok_copy(h, j).start()
                else:
                    @pl.when((mine * per + h != s) | (j != b))
                    def _():
                        tok_copy(h, j).start()

                    @pl.when((mine * per + h == s) & (j == b))
                    def _():
                        tok_recv[mate] = tok_send[h * gb + (j * width) // LANES]

    spots = LANES // width
    spot = b % spots

    def pick(x):
        result = x
        for j in range(1, spots):
            result = jnp.where(spot == j, pltpu.roll(x, LANES - j * width, 1), result)
        return result

    every = nb * R
    lane = lax.broadcasted_iota(jnp.int32, (every, LANES), 1)
    local = (half * gb + (b * width) // LANES) * LANES + lane
    length = stack([len_recv[c] for c in range(nb)])
    rate = -1.0 / stack([hor_recv[c] for c in range(nb)])
    count = jnp.sum(jnp.minimum(length, T).astype(F32), 0, keepdims=True)
    share = 1.0 / count
    jump = jnp.exp(rate * float(L))
    power_out = pick(jnp.exp(rate * (L - 1 - local).astype(F32)))
    valid_out = pick((out_o * L + local < length).astype(F32))
    power = [jnp.exp(rate * (L - 1 - g * LANES - lane).astype(F32)) for g in range(G)]
    power_sum = jnp.broadcast_to(jnp.sum(sum(power[1:], power[0]), 1, keepdims=True), (every, LANES))
    power = [x * x for x in power]
    power_squares = jnp.broadcast_to(jnp.sum(sum(power[1:], power[0]), 1, keepdims=True), (every, LANES))

    part_rows = 2 * rows * (owners - 1) + info_rows
    sum_rows = Q * owners * pairs
    tok_rows = 2 * Q * pairs

    @pl.when(jnp.logical_not(is_owner))
    def _():
        wait_rows(part_rows + 2 * rows + gb * R, sent)
        wait_rows(sum_rows + tok_rows, late)

    @pl.when(own_rw)
    def _():
        wait_rows(part_rows + Q * (n * nb - 1) + 2 * Q * (per * nb - 1), sent)
        wait_rows(sum_rows - Q + tok_rows - 2 * Q, late)

    @pl.when(is_owner & jnp.logical_not(own_rw))
    def _():
        wait_rows(part_rows + gb * R + Q * (n * nb - 1) + 2 * Q * per * nb, sent)
        wait_rows(sum_rows - Q + tok_rows, late)

    gae = pick(stack([tok_recv[c, 0] for c in range(pairs)]))
    values = pick(stack([tok_recv[c, 1] for c in range(pairs)]))
    messages = [stack([sum_recv[o * pairs + c] for c in range(pairs)]) for o in range(owners)]

    def spread(o, i):
        return jnp.broadcast_to(messages[o][:, i:i + 1], (every, LANES))

    u = spread(owners - 1, 0)
    first = sum([spread(o, 1) for o in range(1, owners)], spread(0, 1))
    second = sum([spread(o, 3) for o in range(1, owners)], spread(0, 3))
    entering = jnp.zeros((every, LANES), F32)
    for o in reversed(range(owners - 1)):
        first = first + u * power_sum
        second = second + u * (spread(o, 2) + u * power_squares)
        entering = jnp.where(out_o == o, u, entering)
        if o:
            u = spread(o, 0) + jump * u
    mean = jnp.sum(first, 0, keepdims=True) * share
    var = jnp.maximum(jnp.sum(second, 0, keepdims=True) * share - mean * mean, 1.0)
    scale = lax.rsqrt(var)
    gae = gae + power_out * entering
    out_ref[every:2 * every, :] = ((gae + values) * valid_out)[:, 0:width]
    out_ref[0:every, :] = ((gae - mean) * valid_out * scale)[:, 0:width]


def per_device(hidden, gain, weight, rewards, mask, lengths, horizon):
    n = lax.axis_size("seq")
    nb = lax.axis_size("batch")
    pair = 2 - nb % 2
    owners = n // 2 if n % 4 == 0 else n
    R, T, depth = hidden.shape
    subs = max(T // owners // TILE, 1)
    chunks = owners * subs
    stream = R == 2 and depth == 2 * TILE and T == chunks * TILE
    block = rewards.shape[1]
    per = n // owners
    G = T // owners // LANES
    gb = block // LANES
    rows = G * R
    Q = pair * R
    pairs = nb // pair
    dma = pltpu.SemaphoreType.DMA
    both = pl.pallas_call(
        functools.partial(kernel, n, nb, pair, owners, subs, stream),
        out_shape=pltpu.VMEM((2 * R * nb, block // nb), F32),
        in_specs=[pl.BlockSpec(memory_space=pl.ANY)] * 7,
        out_specs=pl.BlockSpec(memory_space=pltpu.VMEM),
        scratch_shapes=[
            pltpu.VMEM((R, T, depth), jnp.bfloat16),
            pltpu.VMEM((depth,), F32),
            pltpu.VMEM((depth,), F32),
            pltpu.VMEM((R, block), F32),
            pltpu.VMEM((R, block), jnp.int32),
            pltpu.SMEM((R,), jnp.int32),
            pltpu.SMEM((R,), F32),
            pltpu.VMEM((owners, subs, 2, rows // subs, LANES), F32),
            pltpu.VMEM((n * pair, subs, 2, rows // subs, LANES), F32),
            pltpu.VMEM((gb * R, LANES), F32),
            pltpu.VMEM((pair * per, gb * R, LANES), F32),
            pltpu.VMEM((R, LANES), jnp.int32),
            pltpu.VMEM((nb, R, LANES), jnp.int32),
            pltpu.VMEM((R, LANES), F32),
            pltpu.VMEM((nb, R, LANES), F32),
            pltpu.VMEM((Q, LANES), F32),
            pltpu.VMEM((owners * pairs, Q, LANES), F32),
            pltpu.VMEM((G, 2, Q, LANES), F32),
            pltpu.VMEM((pairs, 2, Q, LANES), F32),
            pltpu.VMEM((2 * depth,), F32),
            pltpu.VMEM((2 * R, block), F32),
            pltpu.VMEM((2 * owners * rows + 2 * R * nb + Q * n * nb + 2 * Q * per * nb + rows, LANES), F32),
            pltpu.VMEM((2, R, TILE, LANES), F32),
            dma((chunks,)), dma((4,)), dma(()), dma(()), dma(()), dma(()),
        ],
        compiler_params=pltpu.CompilerParams(collective_id=0, has_side_effects=True),
    )(hidden, gain, weight, rewards, mask, lengths, horizon)
    return both[:R * nb], both[R * nb:]


def solution(mesh):
    return jax.shard_map(
        per_device,
        mesh=mesh,
        in_specs=(
            P("batch", None, "seq"),
            P("seq"),
            P("seq"),
            P("batch", "seq"),
            P("batch", "seq"),
            P("batch"),
            P("batch"),
        ),
        out_specs=(P(None, ("seq", "batch")), P(None, ("seq", "batch"))),
        check_vma=False,
    )
```

```python
import functools

import jax
import jax.numpy as jnp
from jax import lax
from jax.experimental import pallas as pl
from jax.experimental.pallas import tpu as pltpu
from jax.sharding import PartitionSpec as P

EPS = 1e-05
LANES = 128
TILE = 256
F32 = jnp.float32
MESH = pl.DeviceIdType.MESH


def bytes_of(ref, sem):
    return pltpu.make_async_copy(ref, ref, sem)


def stack(pieces):
    return pieces[0] if len(pieces) == 1 else jnp.concatenate(pieces, 0)


def kernel(n, nb, pair, owners, subs, stream, hidden, gain, weight, rewards, mask, lengths, horizon,
           out_ref,
           hv, gain_v, weight_v, rew_v, mask_v, len_s, hor_s,
           part, rbuf, rw_send, rw_recv, len_send, len_recv, hor_send, hor_recv,
           sum_send, sum_recv, tok_send, tok_recv, both_v, both_m, any_rows, held_squares,
           chunk_sem, small_sem, sent, early, part_rs, late):
    R, T, depth = hidden.shape
    block = rewards.shape[1]
    width = block // nb
    per = n // owners
    base = (n - owners) // 2
    L = T // owners
    G = L // LANES
    gb = block // LANES
    rows = G * R
    Q = pair * R
    pairs = nb // pair
    total = depth * n
    s = lax.axis_index("seq")
    b = lax.axis_index("batch")
    side = b % pair
    mate = b // pair
    lead = mate * pair + pair - 1
    is_owner = (s >= base) & (s < base + owners) & (side == pair - 1)
    mine = s - base
    out_o = s // per
    half = s % per
    rw_at = base + out_o

    S = L // subs
    srows = rows // subs
    near_high = s * (owners // 2) // n
    near_low = s % 2

    def turn(k):
        back = owners - 1 - k
        if owners % 2:
            return (s + back) % owners
        return (near_high + back // 2) % (owners // 2) * 2 + (near_low + back) % 2

    def chunk_copy(c, r=slice(None)):
        span = pl.ds(turn(c // subs) * L + c % subs * S, S)
        return pltpu.make_async_copy(hidden.at[r, span, :], hv.at[r, span, :], chunk_sem.at[c])

    def wait_rows(count, sem):
        if count:
            bytes_of(any_rows.at[pl.ds(0, count)], sem).wait()

    smalls = [
        pltpu.make_async_copy(src, dst, small_sem.at[i])
        for i, src, dst in ((0, gain, gain_v), (0, weight, weight_v), (1, rewards, rew_v),
                            (1, mask, mask_v), (2, lengths, len_s), (3, horizon, hor_s))]
    for c in range(owners * subs):
        for r in range(R):
            chunk_copy(c, r).start(priority=int(c > 0))
        if c == 0:
            for copy in smalls:
                copy.start()
    barrier = pltpu.get_barrier_semaphore()
    for k in range(1, nb):
        pl.semaphore_signal(barrier, inc=1, device_id={"batch": lax.rem(b + k, nb)},
                            device_id_type=MESH)

    @pl.when(is_owner)
    def _():
        for k in range(n):
            for c in range(pair):
                if k or c:
                    pl.semaphore_signal(
                        barrier, inc=1,
                        device_id={"seq": (s + k) % n, "batch": mate * pair + (side + c) % pair},
                        device_id_type=MESH)

    def head_pieces():
        bytes_of(both_v.at[pl.ds(0, 2 * depth)], small_sem.at[0]).wait()
        head = (gain_v[...] * weight_v[...]).reshape(1, depth)
        high = head.astype(jnp.bfloat16).astype(F32)
        middle = (head - high).astype(jnp.bfloat16).astype(F32)
        low = head - high - middle
        wrow = lax.broadcasted_iota(jnp.int32, (16, depth), 0)
        pieces = jnp.where(wrow == 0, high, jnp.where(wrow == 1, middle, jnp.where(wrow == 2, low, 0.0)))
        return pieces.astype(jnp.bfloat16)

    def part_copy(o, j):
        return pltpu.make_async_remote_copy(
            part.at[o, j], rbuf.at[s * pair + side, j], sent, part_rs,
            device_id={"seq": base + o, "batch": lead}, device_id_type=MESH)

    def rw_copy():
        return pltpu.make_async_remote_copy(
            rw_send, rw_recv.at[side * per + half], sent, early,
            device_id={"seq": rw_at, "batch": lead}, device_id_type=MESH)

    def info_copy(k, src, dst):
        return pltpu.make_async_remote_copy(
            src, dst.at[b], sent, early,
            device_id={"batch": lax.rem(b + k, nb)}, device_id_type=MESH)

    infos = ((len_send, len_recv), (hor_send, hor_recv))
    own_rw = is_owner & (mine == out_o)

    def send_part(o, j):
        @pl.when(jnp.logical_not(is_owner & (mine == o)))
        def _():
            part_copy(o, j).start()

    pieces = head_pieces()
    bytes_of(both_m, small_sem.at[1]).wait()
    for copy in smalls[4:]:
        copy.wait()
    rw = rew_v[...] * mask_v[...].astype(F32)
    for g in range(gb):
        rw_send[g * R:(g + 1) * R, :] = rw[:, g * LANES:(g + 1) * LANES]
    for r in range(R):
        len_send[r:r + 1, :] = jnp.full((1, LANES), len_s[r], jnp.int32)
        hor_send[r:r + 1, :] = jnp.full((1, LANES), hor_s[r], F32)

    def enter():
        met = jnp.where(is_owner, owners - 1, owners) + nb - 1
        pl.semaphore_wait(barrier, met)

        @pl.when(jnp.logical_not(own_rw))
        def _():
            rw_copy().start()

        for j in range(1, nb):
            for src, dst in infos:
                info_copy(j, src, dst).start()

    def squares_of(h):
        squares = jnp.zeros((h.shape[0], LANES), F32)
        for j in range(depth // LANES):
            wide = h[:, j * LANES:(j + 1) * LANES].astype(F32)
            squares = squares + wide * wide
        return squares

    def compute(k, carry):
        o = turn(k)
        for j in range(subs):
            chunk_copy(k * subs + j).wait()
        for g in range(G):
            for r in range(R):
                at = pl.ds(pl.multiple_of(o * L + g * LANES, LANES), LANES)
                h = hv[r, at, :]
                sums = lax.dot_general(pieces, h, (((1,), (1,)), ((), ())),
                                       preferred_element_type=F32)
                j, row = divmod(g * R + r, srows)
                part[o, j, 0, row:row + 1, :] = jnp.sum(sums[0:8], 0, keepdims=True)
                part[o, j, 1, row:row + 1, :] = jnp.sum(squares_of(h).T, 0, keepdims=True)

        @pl.when(k == 0)
        def _():
            enter()

        for j in range(subs):
            send_part(o, j)
        return carry

    def streamed(*accs):
        for acc in accs:
            pltpu.matmul_pop(acc)
        for step in range(owners * subs + 1):
            if step < owners * subs:
                o, j = turn(step // subs), step % subs
                chunk_copy(step).wait()
                for r in range(R):
                    h = hv[r, pl.ds(pl.multiple_of(o * L + j * S, S), S), :]
                    for m in range(2):
                        cols = slice(m * TILE, (m + 1) * TILE)
                        pltpu.matmul_push_rhs(h[:, cols], staging_register=r, mxu_index=m,
                                              transpose=True)
                        pltpu.matmul_acc_lhs(accs[(step % 2 * R + r) * 2 + m], pieces[:, cols],
                                             load_staged_rhs=r)
                    held_squares[step % 2, r] = squares_of(h)
            if step == 0:
                enter()
            else:
                last = step - 1
                o, j = turn(last // subs), last % subs
                for r in range(R):
                    at = (last % 2 * R + r) * 2
                    sums = pltpu.matmul_pop(accs[at]) + pltpu.matmul_pop(accs[at + 1])
                    sums = jnp.sum(sums[0:8], 0, keepdims=True)
                    for g in range(S // LANES):
                        row = g * R + r
                        square = held_squares[last % 2, r, g * LANES:(g + 1) * LANES, :]
                        part[o, j, 0, row:row + 1, :] = sums[:, g * LANES:(g + 1) * LANES]
                        part[o, j, 1, row:row + 1, :] = jnp.sum(square.T, 0, keepdims=True)
                send_part(o, j)

    if stream:
        pl.run_scoped(streamed, *[pltpu.ACC(i % 2)((16, TILE), F32) for i in range(4 * R)])
    else:
        lax.fori_loop(0, owners, compute, 0)

    @pl.when(own_rw)
    def _():
        rw_recv[side * per + half] = rw_send[...]

    len_recv[b] = len_send[...]
    hor_recv[b] = hor_send[...]
    info_rows = 2 * R * (nb - 1)

    @pl.when(jnp.logical_not(is_owner))
    def _():
        wait_rows(info_rows, early)

    @pl.when(own_rw)
    def _():
        wait_rows(info_rows + gb * R * (pair * per - 1), early)

    @pl.when(is_owner & jnp.logical_not(own_rw))
    def _():
        wait_rows(info_rows + gb * R * pair * per, early)

    def sum_copy(i, j):
        return pltpu.make_async_remote_copy(
            sum_send, sum_recv.at[mine * pairs + mate], sent, late,
            device_id={"seq": i, "batch": j}, device_id_type=MESH)

    def each_sum():
        def one(i):
            for j in range(nb):
                never = isinstance(i, int) and not base <= i < base + owners
                if never or j % pair != pair - 1:
                    sum_copy(i, j).start()
                else:
                    @pl.when((i != s) | (j != b))
                    def _():
                        sum_copy(i, j).start()

        if n * nb <= 32:
            for i in range(n):
                one(i)
        else:
            def body(i, carry):
                one(i)
                return carry
            lax.fori_loop(0, n, body, 0)

    def tok_copy(h, j):
        return pltpu.make_async_remote_copy(
            tok_send.at[h * gb + (j * width) // LANES], tok_recv.at[mate], sent, late,
            device_id={"seq": mine * per + h, "batch": j}, device_id_type=MESH)

    @pl.when(is_owner)
    def _():
        row = lax.broadcasted_iota(jnp.int32, (pair * rows, LANES), 0)
        lane = lax.broadcasted_iota(jnp.int32, (pair * rows, LANES), 1)
        group = row % rows // R
        length = stack([len_recv[mate * pair + c] for c in range(pair) for _ in range(G)])
        reach = stack([hor_recv[mate * pair + c] for c in range(pair) for _ in range(G)])
        rate = -1.0 / reach
        local = group * LANES + lane
        valid = (mine * L + local < length).astype(F32)
        step = 16
        near = [jnp.where(lane < LANES - k, jnp.exp(rate * (k - 1)), 0.0) for k in range(1, step + 1)]
        far = [jnp.where(lane < LANES - k, jnp.exp(rate * k), 0.0) for k in range(step, LANES, step)]
        lead_in = jnp.exp(rate * lane.astype(F32))
        hops = [1 << i for i in range(max(G - 1, 0).bit_length())]
        row_decay = [jnp.where(group + k < G, jnp.exp(rate * (k * LANES)), 0.0) for k in hops]
        into = jnp.where(group < G - 1, jnp.exp(rate * (LANES - 1 - lane).astype(F32)), 0.0)
        power = jnp.exp(rate * (L - 1 - local).astype(F32))
        decay = jnp.exp(rate)
        gains = stack([rw_recv[c * per + h] for c in range(pair) for h in range(per)])

        rbuf[s * pair + side] = part[mine]
        bytes_of(rbuf.at[pl.ds(0, n * pair - 1)], part_rs).wait()
        projected, squares = [], []
        for c in range(pair):
            for j in range(subs):
                first, second = rbuf[c, j, 0], rbuf[c, j, 1]
                for k in range(1, n):
                    first = first + rbuf[k * pair + c, j, 0]
                    second = second + rbuf[k * pair + c, j, 1]
                projected.append(first)
                squares.append(second)
        values = stack(projected) * lax.rsqrt(stack(squares) / total + EPS)
        held = values * valid
        change = (gains - values) * valid
        mixed = decay * change + held
        start = jnp.sum(lead_in * mixed, 1, keepdims=True)
        terms = [factor * pltpu.roll(mixed if k < step else held, LANES - k, 1)
                 for k, factor in enumerate(near, 1)]
        while len(terms) > 1:
            terms = [sum(terms[i + 1:i + 2], terms[i]) for i in range(0, len(terms), 2)]
        gae = change + terms[0]
        terms = [factor * pltpu.roll(gae, LANES - k * step, 1) for k, factor in enumerate(far, 1)]
        while len(terms) > 1:
            terms = [sum(terms[i + 1:i + 2], terms[i]) for i in range(0, len(terms), 2)]
        gae = gae + terms[0]
        start = jnp.broadcast_to(start, gae.shape)
        if G > 1:
            for k, factor in zip(hops, row_decay):
                start = start + factor * pltpu.roll(start, pair * rows - k * R, 0)
            gae = gae + into * pltpu.roll(start, pair * rows - R, 0)
        sums = jnp.where(lane == 1, jnp.sum(gae, 1, keepdims=True), 0.0)
        sums = jnp.where(lane == 2, 2.0 * jnp.sum(gae * power, 1, keepdims=True), sums)
        sums = jnp.where(lane == 3, jnp.sum(gae * gae, 1, keepdims=True), sums)
        sums = jnp.where((lane == 0) & (group == 0), start, sums)
        if G & (G - 1) == 0:
            for k in hops:
                sums = sums + pltpu.roll(sums, pair * rows - k * R, 0)
            for c in range(pair):
                sum_send[c * R:(c + 1) * R, :] = sums[c * rows:c * rows + R]
        else:
            for c in range(pair):
                summary = sums[c * rows:c * rows + R]
                for g in range(1, G):
                    summary = summary + sums[c * rows + g * R:c * rows + (g + 1) * R]
                sum_send[c * R:(c + 1) * R, :] = summary
        sum_recv[mine * pairs + mate] = sum_send[...]
        each_sum()
        for g in range(G):
            for c in range(pair):
                at = c * rows + g * R
                tok_send[g, 0, c * R:(c + 1) * R, :] = gae[at:at + R]
                tok_send[g, 1, c * R:(c + 1) * R, :] = values[at:at + R]
        for h in range(per):
            for j in range(nb):
                if j % pair != pair - 1:
                    tok_copy(h, j).start()
                else:
                    @pl.when((mine * per + h != s) | (j != b))
                    def _():
                        tok_copy(h, j).start()

                    @pl.when((mine * per + h == s) & (j == b))
                    def _():
                        tok_recv[mate] = tok_send[h * gb + (j * width) // LANES]

    spots = LANES // width
    spot = b % spots

    def pick(x):
        result = x
        for j in range(1, spots):
            result = jnp.where(spot == j, pltpu.roll(x, LANES - j * width, 1), result)
        return result

    every = nb * R
    lane = lax.broadcasted_iota(jnp.int32, (every, LANES), 1)
    local = (half * gb + (b * width) // LANES) * LANES + lane
    length = stack([len_recv[c] for c in range(nb)])
    rate = -1.0 / stack([hor_recv[c] for c in range(nb)])
    count = jnp.sum(jnp.minimum(length, T).astype(F32), 0, keepdims=True)
    share = 1.0 / count
    jump = jnp.exp(rate * float(L))
    power_out = pick(jnp.exp(rate * (L - 1 - local).astype(F32)))
    valid_out = pick((out_o * L + local < length).astype(F32))
    power = [jnp.exp(rate * (L - 1 - g * LANES - lane).astype(F32)) for g in range(G)]
    power_sum = jnp.broadcast_to(jnp.sum(sum(power[1:], power[0]), 1, keepdims=True), (every, LANES))
    power = [x * x for x in power]
    power_squares = jnp.broadcast_to(jnp.sum(sum(power[1:], power[0]), 1, keepdims=True), (every, LANES))

    part_rows = 2 * rows * (owners - 1) + info_rows
    sum_rows = Q * owners * pairs
    tok_rows = 2 * Q * pairs

    @pl.when(jnp.logical_not(is_owner))
    def _():
        wait_rows(part_rows + 2 * rows + gb * R, sent)
        wait_rows(sum_rows + tok_rows, late)

    @pl.when(own_rw)
    def _():
        wait_rows(part_rows + Q * (n * nb - 1) + 2 * Q * (per * nb - 1), sent)
        wait_rows(sum_rows - Q + tok_rows - 2 * Q, late)

    @pl.when(is_owner & jnp.logical_not(own_rw))
    def _():
        wait_rows(part_rows + gb * R + Q * (n * nb - 1) + 2 * Q * per * nb, sent)
        wait_rows(sum_rows - Q + tok_rows, late)

    gae = pick(stack([tok_recv[c, 0] for c in range(pairs)]))
    values = pick(stack([tok_recv[c, 1] for c in range(pairs)]))
    messages = [stack([sum_recv[o * pairs + c] for c in range(pairs)]) for o in range(owners)]

    def spread(o, i):
        return jnp.broadcast_to(messages[o][:, i:i + 1], (every, LANES))

    u = spread(owners - 1, 0)
    first = sum([spread(o, 1) for o in range(1, owners)], spread(0, 1))
    second = sum([spread(o, 3) for o in range(1, owners)], spread(0, 3))
    entering = jnp.zeros((every, LANES), F32)
    for o in reversed(range(owners - 1)):
        first = first + u * power_sum
        second = second + u * (spread(o, 2) + u * power_squares)
        entering = jnp.where(out_o == o, u, entering)
        if o:
            u = spread(o, 0) + jump * u
    mean = jnp.sum(first, 0, keepdims=True) * share
    var = jnp.maximum(jnp.sum(second, 0, keepdims=True) * share - mean * mean, 1.0)
    scale = lax.rsqrt(var)
    gae = gae + power_out * entering
    out_ref[every:2 * every, :] = ((gae + values) * valid_out)[:, 0:width]
    out_ref[0:every, :] = ((gae - mean) * valid_out * scale)[:, 0:width]


def per_device(hidden, gain, weight, rewards, mask, lengths, horizon):
    n = lax.axis_size("seq")
    nb = lax.axis_size("batch")
    pair = 2 - nb % 2
    owners = n // 2 if n % 4 == 0 else n
    R, T, depth = hidden.shape
    subs = max(T // owners // TILE, 1)
    chunks = owners * subs
    stream = R == 2 and depth == 2 * TILE and T == chunks * TILE
    block = rewards.shape[1]
    per = n // owners
    G = T // owners // LANES
    gb = block // LANES
    rows = G * R
    Q = pair * R
    pairs = nb // pair
    dma = pltpu.SemaphoreType.DMA
    both = pl.pallas_call(
        functools.partial(kernel, n, nb, pair, owners, subs, stream),
        out_shape=pltpu.VMEM((2 * R * nb, block // nb), F32),
        in_specs=[pl.BlockSpec(memory_space=pl.ANY)] * 7,
        out_specs=pl.BlockSpec(memory_space=pltpu.VMEM),
        scratch_shapes=[
            pltpu.VMEM((R, T, depth), jnp.bfloat16),
            pltpu.VMEM((depth,), F32),
            pltpu.VMEM((depth,), F32),
            pltpu.VMEM((R, block), F32),
            pltpu.VMEM((R, block), jnp.int32),
            pltpu.SMEM((R,), jnp.int32),
            pltpu.SMEM((R,), F32),
            pltpu.VMEM((owners, subs, 2, rows // subs, LANES), F32),
            pltpu.VMEM((n * pair, subs, 2, rows // subs, LANES), F32),
            pltpu.VMEM((gb * R, LANES), F32),
            pltpu.VMEM((pair * per, gb * R, LANES), F32),
            pltpu.VMEM((R, LANES), jnp.int32),
            pltpu.VMEM((nb, R, LANES), jnp.int32),
            pltpu.VMEM((R, LANES), F32),
            pltpu.VMEM((nb, R, LANES), F32),
            pltpu.VMEM((Q, LANES), F32),
            pltpu.VMEM((owners * pairs, Q, LANES), F32),
            pltpu.VMEM((G, 2, Q, LANES), F32),
            pltpu.VMEM((pairs, 2, Q, LANES), F32),
            pltpu.VMEM((2 * depth,), F32),
            pltpu.VMEM((2 * R, block), F32),
            pltpu.VMEM((2 * owners * rows + 2 * R * nb + Q * n * nb + 2 * Q * per * nb + rows, LANES), F32),
            pltpu.VMEM((2, R, TILE, LANES), F32),
            dma((chunks,)), dma((4,)), dma(()), dma(()), dma(()), dma(()),
        ],
        compiler_params=pltpu.CompilerParams(collective_id=0, has_side_effects=True),
    )(hidden, gain, weight, rewards, mask, lengths, horizon)
    return both[:R * nb], both[R * nb:]


def solution(mesh):
    return jax.shard_map(
        per_device,
        mesh=mesh,
        in_specs=(
            P("batch", None, "seq"),
            P("seq"),
            P("seq"),
            P("batch", "seq"),
            P("batch", "seq"),
            P("batch"),
            P("batch"),
        ),
        out_specs=(P(None, ("seq", "batch")), P(None, ("seq", "batch"))),
        check_vma=False,
    )
```

```python
import functools

import jax
import jax.numpy as jnp
from jax import lax
from jax.experimental import pallas as pl
from jax.experimental.pallas import tpu as pltpu
from jax.sharding import PartitionSpec as P

EPS = 1e-05
LANES = 128
TILE = 256
F32 = jnp.float32
MESH = pl.DeviceIdType.MESH


def bytes_of(ref, sem):
    return pltpu.make_async_copy(ref, ref, sem)


def stack(pieces):
    return pieces[0] if len(pieces) == 1 else jnp.concatenate(pieces, 0)


def kernel(n, nb, pair, owners, subs, stream, hidden, gain, weight, rewards, mask, lengths, horizon,
           out_ref,
           hv, gain_v, weight_v, rew_v, mask_v, len_s, hor_s,
           part, rbuf, rw_send, rw_recv, len_send, len_recv, hor_send, hor_recv,
           sum_send, sum_recv, tok_send, tok_recv, small_v, any_rows, held_squares,
           chunk_sem, small_sem, sent, early, part_rs, late):
    R, T, depth = hidden.shape
    block = rewards.shape[1]
    width = block // nb
    per = n // owners
    base = (n - owners) // 2
    L = T // owners
    G = L // LANES
    gb = block // LANES
    rows = G * R
    Q = pair * R
    pairs = nb // pair
    total = depth * n
    s = lax.axis_index("seq")
    b = lax.axis_index("batch")
    side = b % pair
    mate = b // pair
    lead = mate * pair + pair - 1
    is_owner = (s >= base) & (s < base + owners) & (side == pair - 1)
    mine = s - base
    out_o = s // per
    half = s % per
    rw_at = base + out_o

    S = L // subs
    srows = rows // subs
    near_high = s * (owners // 2) // n
    near_low = s % 2

    def turn(k):
        back = owners - 1 - k
        if owners % 2:
            return (s + back) % owners
        return (near_high + back // 2) % (owners // 2) * 2 + (near_low + back) % 2

    def chunk_copy(c, r=slice(None)):
        span = pl.ds(turn(c // subs) * L + c % subs * S, S)
        return pltpu.make_async_copy(hidden.at[r, span, :], hv.at[r, span, :], chunk_sem.at[c])

    def wait_rows(count, sem):
        if count:
            bytes_of(any_rows.at[pl.ds(0, count)], sem).wait()

    smalls = [
        pltpu.make_async_copy(src, dst, small_sem.at[i])
        for i, src, dst in ((0, gain, gain_v), (0, weight, weight_v), (0, rewards, rew_v),
                            (0, mask, mask_v), (1, lengths, len_s), (2, horizon, hor_s))]
    for c in range(owners * subs):
        for r in range(R):
            chunk_copy(c, r).start(priority=int(c > 0))
        if c == 0:
            for copy in smalls:
                copy.start()
    barrier = pltpu.get_barrier_semaphore()
    for k in range(1, nb):
        pl.semaphore_signal(barrier, inc=1, device_id={"batch": lax.rem(b + k, nb)},
                            device_id_type=MESH)

    @pl.when(is_owner)
    def _():
        for k in range(n):
            for c in range(pair):
                if k or c:
                    pl.semaphore_signal(
                        barrier, inc=1,
                        device_id={"seq": (s + k) % n, "batch": mate * pair + (side + c) % pair},
                        device_id_type=MESH)

    def head_pieces():
        head = (gain_v[...] * weight_v[...]).reshape(1, depth)
        high = head.astype(jnp.bfloat16).astype(F32)
        middle = (head - high).astype(jnp.bfloat16).astype(F32)
        low = head - high - middle
        wrow = lax.broadcasted_iota(jnp.int32, (16, depth), 0)
        pieces = jnp.where(wrow == 0, high, jnp.where(wrow == 1, middle, jnp.where(wrow == 2, low, 0.0)))
        return pieces.astype(jnp.bfloat16)

    def part_copy(o, j):
        return pltpu.make_async_remote_copy(
            part.at[o, j], rbuf.at[s * pair + side, j], sent, part_rs,
            device_id={"seq": base + o, "batch": lead}, device_id_type=MESH)

    def rw_copy():
        return pltpu.make_async_remote_copy(
            rw_send, rw_recv.at[side * per + half], sent, early,
            device_id={"seq": rw_at, "batch": lead}, device_id_type=MESH)

    def info_copy(k, src, dst):
        return pltpu.make_async_remote_copy(
            src, dst.at[b], sent, early,
            device_id={"batch": lax.rem(b + k, nb)}, device_id_type=MESH)

    infos = ((len_send, len_recv), (hor_send, hor_recv))
    own_rw = is_owner & (mine == out_o)

    def send_part(o, j):
        @pl.when(jnp.logical_not(is_owner & (mine == o)))
        def _():
            part_copy(o, j).start()

    bytes_of(small_v, small_sem.at[0]).wait()
    pieces = head_pieces()
    for copy in smalls[4:]:
        copy.wait()
    rw = rew_v[...] * mask_v[...].astype(F32)
    for g in range(gb):
        rw_send[g * R:(g + 1) * R, :] = rw[:, g * LANES:(g + 1) * LANES]
    for r in range(R):
        len_send[r:r + 1, :] = jnp.full((1, LANES), len_s[r], jnp.int32)
        hor_send[r:r + 1, :] = jnp.full((1, LANES), hor_s[r], F32)

    def enter():
        met = jnp.where(is_owner, owners - 1, owners) + nb - 1
        pl.semaphore_wait(barrier, met)

        @pl.when(jnp.logical_not(own_rw))
        def _():
            rw_copy().start()

        for j in range(1, nb):
            for src, dst in infos:
                info_copy(j, src, dst).start()

    def squares_of(h):
        squares = jnp.zeros((h.shape[0], LANES), F32)
        for j in range(depth // LANES):
            wide = h[:, j * LANES:(j + 1) * LANES].astype(F32)
            squares = squares + wide * wide
        return squares

    def compute(k, carry):
        o = turn(k)
        for j in range(subs):
            chunk_copy(k * subs + j).wait()
        for g in range(G):
            for r in range(R):
                at = pl.ds(pl.multiple_of(o * L + g * LANES, LANES), LANES)
                h = hv[r, at, :]
                sums = lax.dot_general(pieces, h, (((1,), (1,)), ((), ())),
                                       preferred_element_type=F32)
                j, row = divmod(g * R + r, srows)
                part[o, j, 0, row:row + 1, :] = jnp.sum(sums[0:8], 0, keepdims=True)
                part[o, j, 1, row:row + 1, :] = jnp.sum(squares_of(h).T, 0, keepdims=True)

        @pl.when(k == 0)
        def _():
            enter()

        for j in range(subs):
            send_part(o, j)
        return carry

    def streamed(*accs):
        for acc in accs:
            pltpu.matmul_pop(acc)
        for step in range(owners * subs + 1):
            if step < owners * subs:
                o, j = turn(step // subs), step % subs
                chunk_copy(step).wait()
                for r in range(R):
                    h = hv[r, pl.ds(pl.multiple_of(o * L + j * S, S), S), :]
                    for m in range(2):
                        cols = slice(m * TILE, (m + 1) * TILE)
                        pltpu.matmul_push_rhs(h[:, cols], staging_register=r, mxu_index=m,
                                              transpose=True)
                        pltpu.matmul_acc_lhs(accs[(step % 2 * R + r) * 2 + m], pieces[:, cols],
                                             load_staged_rhs=r)
                    held_squares[step % 2, r] = squares_of(h)
            if step == 0:
                enter()
            else:
                last = step - 1
                o, j = turn(last // subs), last % subs
                for r in range(R):
                    at = (last % 2 * R + r) * 2
                    sums = pltpu.matmul_pop(accs[at]) + pltpu.matmul_pop(accs[at + 1])
                    sums = jnp.sum(sums[0:8], 0, keepdims=True)
                    for g in range(S // LANES):
                        row = g * R + r
                        square = held_squares[last % 2, r, g * LANES:(g + 1) * LANES, :]
                        part[o, j, 0, row:row + 1, :] = sums[:, g * LANES:(g + 1) * LANES]
                        part[o, j, 1, row:row + 1, :] = jnp.sum(square.T, 0, keepdims=True)
                send_part(o, j)

    if stream:
        pl.run_scoped(streamed, *[pltpu.ACC(i % 2)((16, TILE), F32) for i in range(4 * R)])
    else:
        lax.fori_loop(0, owners, compute, 0)

    @pl.when(own_rw)
    def _():
        rw_recv[side * per + half] = rw_send[...]

    len_recv[b] = len_send[...]
    hor_recv[b] = hor_send[...]
    info_rows = 2 * R * (nb - 1)

    @pl.when(jnp.logical_not(is_owner))
    def _():
        wait_rows(info_rows, early)

    @pl.when(own_rw)
    def _():
        wait_rows(info_rows + gb * R * (pair * per - 1), early)

    @pl.when(is_owner & jnp.logical_not(own_rw))
    def _():
        wait_rows(info_rows + gb * R * pair * per, early)

    def sum_copy(i, j):
        return pltpu.make_async_remote_copy(
            sum_send, sum_recv.at[mine * pairs + mate], sent, late,
            device_id={"seq": i, "batch": j}, device_id_type=MESH)

    def each_sum():
        def one(i):
            for j in range(nb):
                never = isinstance(i, int) and not base <= i < base + owners
                if never or j % pair != pair - 1:
                    sum_copy(i, j).start()
                else:
                    @pl.when((i != s) | (j != b))
                    def _():
                        sum_copy(i, j).start()

        if n * nb <= 32:
            for i in range(n):
                one(i)
        else:
            def body(i, carry):
                one(i)
                return carry
            lax.fori_loop(0, n, body, 0)

    def tok_copy(h, j):
        return pltpu.make_async_remote_copy(
            tok_send.at[h * gb + (j * width) // LANES], tok_recv.at[mate], sent, late,
            device_id={"seq": mine * per + h, "batch": j}, device_id_type=MESH)

    @pl.when(is_owner)
    def _():
        row = lax.broadcasted_iota(jnp.int32, (pair * rows, LANES), 0)
        lane = lax.broadcasted_iota(jnp.int32, (pair * rows, LANES), 1)
        group = row % rows // R
        length = stack([len_recv[mate * pair + c] for c in range(pair) for _ in range(G)])
        reach = stack([hor_recv[mate * pair + c] for c in range(pair) for _ in range(G)])
        rate = -1.0 / reach
        local = group * LANES + lane
        valid = (mine * L + local < length).astype(F32)
        step = 16
        near = [jnp.where(lane < LANES - k, jnp.exp(rate * (k - 1)), 0.0) for k in range(1, step + 1)]
        far = [jnp.where(lane < LANES - k, jnp.exp(rate * k), 0.0) for k in range(step, LANES, step)]
        lead_in = jnp.exp(rate * lane.astype(F32))
        hops = [1 << i for i in range(max(G - 1, 0).bit_length())]
        row_decay = [jnp.where(group + k < G, jnp.exp(rate * (k * LANES)), 0.0) for k in hops]
        into = jnp.where(group < G - 1, jnp.exp(rate * (LANES - 1 - lane).astype(F32)), 0.0)
        power = jnp.exp(rate * (L - 1 - local).astype(F32))
        decay = jnp.exp(rate)
        gains = stack([rw_recv[c * per + h] for c in range(pair) for h in range(per)])

        rbuf[s * pair + side] = part[mine]
        bytes_of(rbuf.at[pl.ds(0, n * pair - 1)], part_rs).wait()
        projected, squares = [], []
        for c in range(pair):
            for j in range(subs):
                first, second = rbuf[c, j, 0], rbuf[c, j, 1]
                for k in range(1, n):
                    first = first + rbuf[k * pair + c, j, 0]
                    second = second + rbuf[k * pair + c, j, 1]
                projected.append(first)
                squares.append(second)
        values = stack(projected) * lax.rsqrt(stack(squares) / total + EPS)
        held = values * valid
        change = (gains - values) * valid
        mixed = decay * change + held
        start = jnp.sum(lead_in * mixed, 1, keepdims=True)
        terms = [factor * pltpu.roll(mixed if k < step else held, LANES - k, 1)
                 for k, factor in enumerate(near, 1)]
        while len(terms) > 1:
            terms = [sum(terms[i + 1:i + 2], terms[i]) for i in range(0, len(terms), 2)]
        gae = change + terms[0]
        terms = [factor * pltpu.roll(gae, LANES - k * step, 1) for k, factor in enumerate(far, 1)]
        while len(terms) > 1:
            terms = [sum(terms[i + 1:i + 2], terms[i]) for i in range(0, len(terms), 2)]
        gae = gae + terms[0]
        start = jnp.broadcast_to(start, gae.shape)
        if G > 1:
            for k, factor in zip(hops, row_decay):
                start = start + factor * pltpu.roll(start, pair * rows - k * R, 0)
            gae = gae + into * pltpu.roll(start, pair * rows - R, 0)
        sums = jnp.where(lane == 1, jnp.sum(gae, 1, keepdims=True), 0.0)
        sums = jnp.where(lane == 2, 2.0 * jnp.sum(gae * power, 1, keepdims=True), sums)
        sums = jnp.where(lane == 3, jnp.sum(gae * gae, 1, keepdims=True), sums)
        sums = jnp.where((lane == 0) & (group == 0), start, sums)
        if G & (G - 1) == 0:
            for k in hops:
                sums = sums + pltpu.roll(sums, pair * rows - k * R, 0)
            for c in range(pair):
                sum_send[c * R:(c + 1) * R, :] = sums[c * rows:c * rows + R]
        else:
            for c in range(pair):
                summary = sums[c * rows:c * rows + R]
                for g in range(1, G):
                    summary = summary + sums[c * rows + g * R:c * rows + (g + 1) * R]
                sum_send[c * R:(c + 1) * R, :] = summary
        sum_recv[mine * pairs + mate] = sum_send[...]
        each_sum()
        for g in range(G):
            for c in range(pair):
                at = c * rows + g * R
                tok_send[g, 0, c * R:(c + 1) * R, :] = gae[at:at + R]
                tok_send[g, 1, c * R:(c + 1) * R, :] = values[at:at + R]
        for h in range(per):
            for j in range(nb):
                if j % pair != pair - 1:
                    tok_copy(h, j).start()
                else:
                    @pl.when((mine * per + h != s) | (j != b))
                    def _():
                        tok_copy(h, j).start()

                    @pl.when((mine * per + h == s) & (j == b))
                    def _():
                        tok_recv[mate] = tok_send[h * gb + (j * width) // LANES]

    spots = LANES // width
    spot = b % spots

    def pick(x):
        result = x
        for j in range(1, spots):
            result = jnp.where(spot == j, pltpu.roll(x, LANES - j * width, 1), result)
        return result

    every = nb * R
    lane = lax.broadcasted_iota(jnp.int32, (every, LANES), 1)
    local = (half * gb + (b * width) // LANES) * LANES + lane
    length = stack([len_recv[c] for c in range(nb)])
    rate = -1.0 / stack([hor_recv[c] for c in range(nb)])
    count = jnp.sum(jnp.minimum(length, T).astype(F32), 0, keepdims=True)
    share = 1.0 / count
    jump = jnp.exp(rate * float(L))
    power_out = pick(jnp.exp(rate * (L - 1 - local).astype(F32)))
    valid_out = pick((out_o * L + local < length).astype(F32))
    power = [jnp.exp(rate * (L - 1 - g * LANES - lane).astype(F32)) for g in range(G)]
    power_sum = jnp.broadcast_to(jnp.sum(sum(power[1:], power[0]), 1, keepdims=True), (every, LANES))
    power = [x * x for x in power]
    power_squares = jnp.broadcast_to(jnp.sum(sum(power[1:], power[0]), 1, keepdims=True), (every, LANES))

    part_rows = 2 * rows * (owners - 1) + info_rows
    sum_rows = Q * owners * pairs
    tok_rows = 2 * Q * pairs

    @pl.when(jnp.logical_not(is_owner))
    def _():
        wait_rows(part_rows + 2 * rows + gb * R, sent)
        wait_rows(sum_rows + tok_rows, late)

    @pl.when(own_rw)
    def _():
        wait_rows(part_rows + Q * (n * nb - 1) + 2 * Q * (per * nb - 1), sent)
        wait_rows(sum_rows - Q + tok_rows - 2 * Q, late)

    @pl.when(is_owner & jnp.logical_not(own_rw))
    def _():
        wait_rows(part_rows + gb * R + Q * (n * nb - 1) + 2 * Q * per * nb, sent)
        wait_rows(sum_rows - Q + tok_rows, late)

    gae = pick(stack([tok_recv[c, 0] for c in range(pairs)]))
    values = pick(stack([tok_recv[c, 1] for c in range(pairs)]))
    messages = [stack([sum_recv[o * pairs + c] for c in range(pairs)]) for o in range(owners)]

    def spread(o, i):
        return jnp.broadcast_to(messages[o][:, i:i + 1], (every, LANES))

    u = spread(owners - 1, 0)
    first = sum([spread(o, 1) for o in range(1, owners)], spread(0, 1))
    second = sum([spread(o, 3) for o in range(1, owners)], spread(0, 3))
    entering = jnp.zeros((every, LANES), F32)
    for o in reversed(range(owners - 1)):
        first = first + u * power_sum
        second = second + u * (spread(o, 2) + u * power_squares)
        entering = jnp.where(out_o == o, u, entering)
        if o:
            u = spread(o, 0) + jump * u
    mean = jnp.sum(first, 0, keepdims=True) * share
    var = jnp.maximum(jnp.sum(second, 0, keepdims=True) * share - mean * mean, 1.0)
    scale = lax.rsqrt(var)
    gae = gae + power_out * entering
    out_ref[every:2 * every, :] = ((gae + values) * valid_out)[:, 0:width]
    out_ref[0:every, :] = ((gae - mean) * valid_out * scale)[:, 0:width]


def per_device(hidden, gain, weight, rewards, mask, lengths, horizon):
    n = lax.axis_size("seq")
    nb = lax.axis_size("batch")
    pair = 2 - nb % 2
    owners = n // 2 if n % 4 == 0 else n
    R, T, depth = hidden.shape
    subs = max(T // owners // TILE, 1)
    chunks = owners * subs
    stream = R == 2 and depth == 2 * TILE and T == chunks * TILE
    block = rewards.shape[1]
    per = n // owners
    G = T // owners // LANES
    gb = block // LANES
    rows = G * R
    Q = pair * R
    pairs = nb // pair
    dma = pltpu.SemaphoreType.DMA
    both = pl.pallas_call(
        functools.partial(kernel, n, nb, pair, owners, subs, stream),
        out_shape=pltpu.VMEM((2 * R * nb, block // nb), F32),
        in_specs=[pl.BlockSpec(memory_space=pl.ANY)] * 7,
        out_specs=pl.BlockSpec(memory_space=pltpu.VMEM),
        scratch_shapes=[
            pltpu.VMEM((R, T, depth), jnp.bfloat16),
            pltpu.VMEM((depth,), F32),
            pltpu.VMEM((depth,), F32),
            pltpu.VMEM((R, block), F32),
            pltpu.VMEM((R, block), jnp.int32),
            pltpu.SMEM((R,), jnp.int32),
            pltpu.SMEM((R,), F32),
            pltpu.VMEM((owners, subs, 2, rows // subs, LANES), F32),
            pltpu.VMEM((n * pair, subs, 2, rows // subs, LANES), F32),
            pltpu.VMEM((gb * R, LANES), F32),
            pltpu.VMEM((pair * per, gb * R, LANES), F32),
            pltpu.VMEM((R, LANES), jnp.int32),
            pltpu.VMEM((nb, R, LANES), jnp.int32),
            pltpu.VMEM((R, LANES), F32),
            pltpu.VMEM((nb, R, LANES), F32),
            pltpu.VMEM((Q, LANES), F32),
            pltpu.VMEM((owners * pairs, Q, LANES), F32),
            pltpu.VMEM((G, 2, Q, LANES), F32),
            pltpu.VMEM((pairs, 2, Q, LANES), F32),
            pltpu.VMEM((2 * depth + 2 * R * block,), F32),
            pltpu.VMEM((2 * owners * rows + 2 * R * nb + Q * n * nb + 2 * Q * per * nb + rows, LANES), F32),
            pltpu.VMEM((2, R, TILE, LANES), F32),
            dma((chunks,)), dma((3,)), dma(()), dma(()), dma(()), dma(()),
        ],
        compiler_params=pltpu.CompilerParams(collective_id=0, has_side_effects=True),
    )(hidden, gain, weight, rewards, mask, lengths, horizon)
    return both[:R * nb], both[R * nb:]


def solution(mesh):
    return jax.shard_map(
        per_device,
        mesh=mesh,
        in_specs=(
            P("batch", None, "seq"),
            P("seq"),
            P("seq"),
            P("batch", "seq"),
            P("batch", "seq"),
            P("batch"),
            P("batch"),
        ),
        out_specs=(P(None, ("seq", "batch")), P(None, ("seq", "batch"))),
        check_vma=False,
    )
```

```python
import functools

import jax
import jax.numpy as jnp
from jax import lax
from jax.experimental import pallas as pl
from jax.experimental.pallas import tpu as pltpu
from jax.sharding import PartitionSpec as P

EPS = 1e-05
LANES = 128
TILE = 256
F32 = jnp.float32
MESH = pl.DeviceIdType.MESH


def bytes_of(ref, sem):
    return pltpu.make_async_copy(ref, ref, sem)


def stack(pieces):
    return pieces[0] if len(pieces) == 1 else jnp.concatenate(pieces, 0)


def kernel(n, nb, pair, owners, subs, stream, hidden, gain, weight, rewards, mask, lengths, horizon,
           out_ref,
           hv, gain_v, weight_v, rew_v, mask_v, len_s, hor_s,
           part, rbuf, rw_send, rw_recv, len_send, len_recv, hor_send, hor_recv,
           sum_send, sum_recv, tok_send, tok_recv, small_v, any_rows, held_squares,
           chunk_sem, small_sem, early, part_rs, late):
    R, T, depth = hidden.shape
    block = rewards.shape[1]
    width = block // nb
    per = n // owners
    base = (n - owners) // 2
    L = T // owners
    G = L // LANES
    gb = block // LANES
    rows = G * R
    Q = pair * R
    pairs = nb // pair
    total = depth * n
    s = lax.axis_index("seq")
    b = lax.axis_index("batch")
    side = b % pair
    mate = b // pair
    lead = mate * pair + pair - 1
    is_owner = (s >= base) & (s < base + owners) & (side == pair - 1)
    mine = s - base
    out_o = s // per
    half = s % per
    rw_at = base + out_o

    S = L // subs
    sent = small_sem.at[0]
    srows = rows // subs
    near_high = s * (owners // 2) // n
    near_low = s % 2

    def turn(k):
        back = owners - 1 - k
        if owners % 2:
            return (s + back) % owners
        return (near_high + back // 2) % (owners // 2) * 2 + (near_low + back) % 2

    def chunk_copy(c, r=slice(None)):
        span = pl.ds(turn(c // subs) * L + c % subs * S, S)
        return pltpu.make_async_copy(hidden.at[r, span, :], hv.at[r, span, :], chunk_sem.at[c])

    def wait_rows(count, sem):
        if count:
            bytes_of(any_rows.at[pl.ds(0, count)], sem).wait()

    smalls = [
        pltpu.make_async_copy(src, dst, small_sem.at[i])
        for i, src, dst in ((0, gain, gain_v), (0, weight, weight_v), (0, rewards, rew_v),
                            (0, mask, mask_v), (1, lengths, len_s), (2, horizon, hor_s))]
    for c in range(owners * subs):
        for r in range(R):
            chunk_copy(c, r).start(priority=int(c > 0))
        if c == 0:
            for copy in smalls:
                copy.start()
    barrier = pltpu.get_barrier_semaphore()
    for k in range(1, nb):
        pl.semaphore_signal(barrier, inc=1, device_id={"batch": lax.rem(b + k, nb)},
                            device_id_type=MESH)

    @pl.when(is_owner)
    def _():
        for k in range(n):
            for c in range(pair):
                if k or c:
                    pl.semaphore_signal(
                        barrier, inc=1,
                        device_id={"seq": (s + k) % n, "batch": mate * pair + (side + c) % pair},
                        device_id_type=MESH)

    def head_pieces():
        head = (gain_v[...] * weight_v[...]).reshape(1, depth)
        high = head.astype(jnp.bfloat16).astype(F32)
        middle = (head - high).astype(jnp.bfloat16).astype(F32)
        low = head - high - middle
        wrow = lax.broadcasted_iota(jnp.int32, (16, depth), 0)
        pieces = jnp.where(wrow == 0, high, jnp.where(wrow == 1, middle, jnp.where(wrow == 2, low, 0.0)))
        return pieces.astype(jnp.bfloat16)

    def part_copy(o, j):
        return pltpu.make_async_remote_copy(
            part.at[o, j], rbuf.at[s * pair + side, j], sent, part_rs,
            device_id={"seq": base + o, "batch": lead}, device_id_type=MESH)

    def rw_copy():
        return pltpu.make_async_remote_copy(
            rw_send, rw_recv.at[side * per + half], sent, early,
            device_id={"seq": rw_at, "batch": lead}, device_id_type=MESH)

    def info_copy(k, src, dst):
        return pltpu.make_async_remote_copy(
            src, dst.at[b], sent, early,
            device_id={"batch": lax.rem(b + k, nb)}, device_id_type=MESH)

    infos = ((len_send, len_recv), (hor_send, hor_recv))
    own_rw = is_owner & (mine == out_o)

    def send_part(o, j):
        @pl.when(jnp.logical_not(is_owner & (mine == o)))
        def _():
            part_copy(o, j).start()

    bytes_of(small_v, small_sem.at[0]).wait()
    pieces = head_pieces()
    for copy in smalls[4:]:
        copy.wait()
    rw = rew_v[...] * mask_v[...].astype(F32)
    for g in range(gb):
        rw_send[g * R:(g + 1) * R, :] = rw[:, g * LANES:(g + 1) * LANES]
    for r in range(R):
        len_send[r:r + 1, :] = jnp.full((1, LANES), len_s[r], jnp.int32)
        hor_send[r:r + 1, :] = jnp.full((1, LANES), hor_s[r], F32)

    def enter():
        met = jnp.where(is_owner, owners - 1, owners) + nb - 1
        pl.semaphore_wait(barrier, met)

        @pl.when(jnp.logical_not(own_rw))
        def _():
            rw_copy().start()

        for j in range(1, nb):
            for src, dst in infos:
                info_copy(j, src, dst).start()

    def squares_of(h):
        squares = jnp.zeros((h.shape[0], LANES), F32)
        for j in range(depth // LANES):
            wide = h[:, j * LANES:(j + 1) * LANES].astype(F32)
            squares = squares + wide * wide
        return squares

    def compute(k, carry):
        o = turn(k)
        for j in range(subs):
            chunk_copy(k * subs + j).wait()
        for g in range(G):
            for r in range(R):
                at = pl.ds(pl.multiple_of(o * L + g * LANES, LANES), LANES)
                h = hv[r, at, :]
                sums = lax.dot_general(pieces, h, (((1,), (1,)), ((), ())),
                                       preferred_element_type=F32)
                j, row = divmod(g * R + r, srows)
                part[o, j, 0, row:row + 1, :] = jnp.sum(sums[0:8], 0, keepdims=True)
                part[o, j, 1, row:row + 1, :] = jnp.sum(squares_of(h).T, 0, keepdims=True)

        @pl.when(k == 0)
        def _():
            enter()

        for j in range(subs):
            send_part(o, j)
        return carry

    def streamed(*accs):
        for acc in accs:
            pltpu.matmul_pop(acc)
        for step in range(owners * subs + 1):
            if step < owners * subs:
                o, j = turn(step // subs), step % subs
                chunk_copy(step).wait()
                for r in range(R):
                    h = hv[r, pl.ds(pl.multiple_of(o * L + j * S, S), S), :]
                    for m in range(2):
                        cols = slice(m * TILE, (m + 1) * TILE)
                        pltpu.matmul_push_rhs(h[:, cols], staging_register=r, mxu_index=m,
                                              transpose=True)
                        pltpu.matmul_acc_lhs(accs[(step % 2 * R + r) * 2 + m], pieces[:, cols],
                                             load_staged_rhs=r)
                    held_squares[step % 2, r] = squares_of(h)
            if step == 0:
                enter()
            else:
                last = step - 1
                o, j = turn(last // subs), last % subs
                for r in range(R):
                    at = (last % 2 * R + r) * 2
                    sums = pltpu.matmul_pop(accs[at]) + pltpu.matmul_pop(accs[at + 1])
                    sums = jnp.sum(sums[0:8], 0, keepdims=True)
                    for g in range(S // LANES):
                        row = g * R + r
                        square = held_squares[last % 2, r, g * LANES:(g + 1) * LANES, :]
                        part[o, j, 0, row:row + 1, :] = sums[:, g * LANES:(g + 1) * LANES]
                        part[o, j, 1, row:row + 1, :] = jnp.sum(square.T, 0, keepdims=True)
                send_part(o, j)

    if stream:
        pl.run_scoped(streamed, *[pltpu.ACC(i % 2)((16, TILE), F32) for i in range(4 * R)])
    else:
        lax.fori_loop(0, owners, compute, 0)

    @pl.when(own_rw)
    def _():
        rw_recv[side * per + half] = rw_send[...]

    len_recv[b] = len_send[...]
    hor_recv[b] = hor_send[...]
    info_rows = 2 * R * (nb - 1)

    @pl.when(jnp.logical_not(is_owner))
    def _():
        wait_rows(info_rows, early)

    @pl.when(own_rw)
    def _():
        wait_rows(info_rows + gb * R * (pair * per - 1), early)

    @pl.when(is_owner & jnp.logical_not(own_rw))
    def _():
        wait_rows(info_rows + gb * R * pair * per, early)

    def sum_copy(i, j):
        return pltpu.make_async_remote_copy(
            sum_send, sum_recv.at[mine * pairs + mate], sent, late,
            device_id={"seq": i, "batch": j}, device_id_type=MESH)

    def each_sum():
        def one(i):
            for j in range(nb):
                never = isinstance(i, int) and not base <= i < base + owners
                if never or j % pair != pair - 1:
                    sum_copy(i, j).start()
                else:
                    @pl.when((i != s) | (j != b))
                    def _():
                        sum_copy(i, j).start()

        if n * nb <= 32:
            for i in range(n):
                one(i)
        else:
            def body(i, carry):
                one(i)
                return carry
            lax.fori_loop(0, n, body, 0)

    def tok_copy(h, j):
        return pltpu.make_async_remote_copy(
            tok_send.at[h * gb + (j * width) // LANES], tok_recv.at[mate], sent, late,
            device_id={"seq": mine * per + h, "batch": j}, device_id_type=MESH)

    @pl.when(is_owner)
    def _():
        row = lax.broadcasted_iota(jnp.int32, (pair * rows, LANES), 0)
        lane = lax.broadcasted_iota(jnp.int32, (pair * rows, LANES), 1)
        group = row % rows // R
        length = stack([len_recv[mate * pair + c] for c in range(pair) for _ in range(G)])
        reach = stack([hor_recv[mate * pair + c] for c in range(pair) for _ in range(G)])
        rate = -1.0 / reach
        local = group * LANES + lane
        valid = (mine * L + local < length).astype(F32)
        step = 16
        near = [jnp.where(lane < LANES - k, jnp.exp(rate * (k - 1)), 0.0) for k in range(1, step + 1)]
        far = [jnp.where(lane < LANES - k, jnp.exp(rate * k), 0.0) for k in range(step, LANES, step)]
        lead_in = jnp.exp(rate * lane.astype(F32))
        hops = [1 << i for i in range(max(G - 1, 0).bit_length())]
        row_decay = [jnp.where(group + k < G, jnp.exp(rate * (k * LANES)), 0.0) for k in hops]
        into = jnp.where(group < G - 1, jnp.exp(rate * (LANES - 1 - lane).astype(F32)), 0.0)
        power = jnp.exp(rate * (L - 1 - local).astype(F32))
        decay = jnp.exp(rate)
        gains = stack([rw_recv[c * per + h] for c in range(pair) for h in range(per)])

        rbuf[s * pair + side] = part[mine]
        bytes_of(rbuf.at[pl.ds(0, n * pair - 1)], part_rs).wait()
        projected, squares = [], []
        for c in range(pair):
            for j in range(subs):
                first, second = rbuf[c, j, 0], rbuf[c, j, 1]
                for k in range(1, n):
                    first = first + rbuf[k * pair + c, j, 0]
                    second = second + rbuf[k * pair + c, j, 1]
                projected.append(first)
                squares.append(second)
        values = stack(projected) * lax.rsqrt(stack(squares) / total + EPS)
        held = values * valid
        change = (gains - values) * valid
        mixed = decay * change + held
        start = jnp.sum(lead_in * mixed, 1, keepdims=True)
        terms = [factor * pltpu.roll(mixed if k < step else held, LANES - k, 1)
                 for k, factor in enumerate(near, 1)]
        while len(terms) > 1:
            terms = [sum(terms[i + 1:i + 2], terms[i]) for i in range(0, len(terms), 2)]
        gae = change + terms[0]
        terms = [factor * pltpu.roll(gae, LANES - k * step, 1) for k, factor in enumerate(far, 1)]
        while len(terms) > 1:
            terms = [sum(terms[i + 1:i + 2], terms[i]) for i in range(0, len(terms), 2)]
        gae = gae + terms[0]
        start = jnp.broadcast_to(start, gae.shape)
        if G > 1:
            for k, factor in zip(hops, row_decay):
                start = start + factor * pltpu.roll(start, pair * rows - k * R, 0)
            gae = gae + into * pltpu.roll(start, pair * rows - R, 0)
        sums = jnp.where(lane == 1, jnp.sum(gae, 1, keepdims=True), 0.0)
        sums = jnp.where(lane == 2, 2.0 * jnp.sum(gae * power, 1, keepdims=True), sums)
        sums = jnp.where(lane == 3, jnp.sum(gae * gae, 1, keepdims=True), sums)
        sums = jnp.where((lane == 0) & (group == 0), start, sums)
        if G & (G - 1) == 0:
            for k in hops:
                sums = sums + pltpu.roll(sums, pair * rows - k * R, 0)
            for c in range(pair):
                sum_send[c * R:(c + 1) * R, :] = sums[c * rows:c * rows + R]
        else:
            for c in range(pair):
                summary = sums[c * rows:c * rows + R]
                for g in range(1, G):
                    summary = summary + sums[c * rows + g * R:c * rows + (g + 1) * R]
                sum_send[c * R:(c + 1) * R, :] = summary
        each_sum()
        sum_recv[mine * pairs + mate] = sum_send[...]
        for g in range(G):
            for c in range(pair):
                at = c * rows + g * R
                tok_send[g, 0, c * R:(c + 1) * R, :] = gae[at:at + R]
                tok_send[g, 1, c * R:(c + 1) * R, :] = values[at:at + R]
        for h in range(per):
            for j in range(nb):
                if j % pair != pair - 1:
                    tok_copy(h, j).start()
                else:
                    @pl.when((mine * per + h != s) | (j != b))
                    def _():
                        tok_copy(h, j).start()

                    @pl.when((mine * per + h == s) & (j == b))
                    def _():
                        tok_recv[mate] = tok_send[h * gb + (j * width) // LANES]

    spots = LANES // width
    spot = b % spots

    def pick(x):
        result = x
        for j in range(1, spots):
            result = jnp.where(spot == j, pltpu.roll(x, LANES - j * width, 1), result)
        return result

    every = nb * R
    lane = lax.broadcasted_iota(jnp.int32, (every, LANES), 1)
    local = (half * gb + (b * width) // LANES) * LANES + lane
    length = stack([len_recv[c] for c in range(nb)])
    rate = -1.0 / stack([hor_recv[c] for c in range(nb)])
    count = jnp.sum(jnp.minimum(length, T).astype(F32), 0, keepdims=True)
    share = 1.0 / count
    jump = jnp.exp(rate * float(L))
    power_out = pick(jnp.exp(rate * (L - 1 - local).astype(F32)))
    valid_out = pick((out_o * L + local < length).astype(F32))
    power = [jnp.exp(rate * (L - 1 - g * LANES - lane).astype(F32)) for g in range(G)]
    power_sum = jnp.broadcast_to(jnp.sum(sum(power[1:], power[0]), 1, keepdims=True), (every, LANES))
    power = [x * x for x in power]
    power_squares = jnp.broadcast_to(jnp.sum(sum(power[1:], power[0]), 1, keepdims=True), (every, LANES))

    part_rows = 2 * rows * (owners - 1) + info_rows
    sum_rows = Q * owners * pairs
    tok_rows = 2 * Q * pairs

    @pl.when(jnp.logical_not(is_owner))
    def _():
        wait_rows(part_rows + 2 * rows + gb * R, sent)
        wait_rows(sum_rows + tok_rows, late)

    @pl.when(own_rw)
    def _():
        wait_rows(part_rows + Q * (n * nb - 1) + 2 * Q * (per * nb - 1), sent)
        wait_rows(sum_rows - Q + tok_rows - 2 * Q, late)

    @pl.when(is_owner & jnp.logical_not(own_rw))
    def _():
        wait_rows(part_rows + gb * R + Q * (n * nb - 1) + 2 * Q * per * nb, sent)
        wait_rows(sum_rows - Q + tok_rows, late)

    gae = pick(stack([tok_recv[c, 0] for c in range(pairs)]))
    values = pick(stack([tok_recv[c, 1] for c in range(pairs)]))
    messages = [stack([sum_recv[o * pairs + c] for c in range(pairs)]) for o in range(owners)]

    def spread(o, i):
        return jnp.broadcast_to(messages[o][:, i:i + 1], (every, LANES))

    u = spread(owners - 1, 0)
    first = sum([spread(o, 1) for o in range(1, owners)], spread(0, 1))
    second = sum([spread(o, 3) for o in range(1, owners)], spread(0, 3))
    entering = jnp.zeros((every, LANES), F32)
    for o in reversed(range(owners - 1)):
        first = first + u * power_sum
        second = second + u * (spread(o, 2) + u * power_squares)
        entering = jnp.where(out_o == o, u, entering)
        if o:
            u = spread(o, 0) + jump * u
    mean = jnp.sum(first, 0, keepdims=True) * share
    var = jnp.maximum(jnp.sum(second, 0, keepdims=True) * share - mean * mean, 1.0)
    scale = lax.rsqrt(var)
    gae = gae + power_out * entering
    out_ref[every:2 * every, :] = ((gae + values) * valid_out)[:, 0:width]
    out_ref[0:every, :] = ((gae - mean) * valid_out * scale)[:, 0:width]


def per_device(hidden, gain, weight, rewards, mask, lengths, horizon):
    n = lax.axis_size("seq")
    nb = lax.axis_size("batch")
    pair = 2 - nb % 2
    owners = n // 2 if n % 4 == 0 else n
    R, T, depth = hidden.shape
    subs = max(T // owners // TILE, 1)
    chunks = owners * subs
    stream = R == 2 and depth == 2 * TILE and T == chunks * TILE
    block = rewards.shape[1]
    per = n // owners
    G = T // owners // LANES
    gb = block // LANES
    rows = G * R
    Q = pair * R
    pairs = nb // pair
    dma = pltpu.SemaphoreType.DMA
    both = pl.pallas_call(
        functools.partial(kernel, n, nb, pair, owners, subs, stream),
        out_shape=pltpu.VMEM((2 * R * nb, block // nb), F32),
        in_specs=[pl.BlockSpec(memory_space=pl.ANY)] * 7,
        out_specs=pl.BlockSpec(memory_space=pltpu.VMEM),
        scratch_shapes=[
            pltpu.VMEM((R, T, depth), jnp.bfloat16),
            pltpu.VMEM((depth,), F32),
            pltpu.VMEM((depth,), F32),
            pltpu.VMEM((R, block), F32),
            pltpu.VMEM((R, block), jnp.int32),
            pltpu.SMEM((R,), jnp.int32),
            pltpu.SMEM((R,), F32),
            pltpu.VMEM((owners, subs, 2, rows // subs, LANES), F32),
            pltpu.VMEM((n * pair, subs, 2, rows // subs, LANES), F32),
            pltpu.VMEM((gb * R, LANES), F32),
            pltpu.VMEM((pair * per, gb * R, LANES), F32),
            pltpu.VMEM((R, LANES), jnp.int32),
            pltpu.VMEM((nb, R, LANES), jnp.int32),
            pltpu.VMEM((R, LANES), F32),
            pltpu.VMEM((nb, R, LANES), F32),
            pltpu.VMEM((Q, LANES), F32),
            pltpu.VMEM((owners * pairs, Q, LANES), F32),
            pltpu.VMEM((G, 2, Q, LANES), F32),
            pltpu.VMEM((pairs, 2, Q, LANES), F32),
            pltpu.VMEM((2 * depth + 2 * R * block,), F32),
            pltpu.VMEM((2 * owners * rows + 2 * R * nb + Q * n * nb + 2 * Q * per * nb + rows, LANES), F32),
            pltpu.VMEM((2, R, TILE, LANES), F32),
            dma((chunks,)), dma((3,)), dma(()), dma(()), dma(()),
        ],
        compiler_params=pltpu.CompilerParams(collective_id=0, has_side_effects=True),
    )(hidden, gain, weight, rewards, mask, lengths, horizon)
    return both[:R * nb], both[R * nb:]


def solution(mesh):
    return jax.shard_map(
        per_device,
        mesh=mesh,
        in_specs=(
            P("batch", None, "seq"),
            P("seq"),
            P("seq"),
            P("batch", "seq"),
            P("batch", "seq"),
            P("batch"),
            P("batch"),
        ),
        out_specs=(P(None, ("seq", "batch")), P(None, ("seq", "batch"))),
        check_vma=False,
    )
```

```python
import functools

import jax
import jax.numpy as jnp
from jax import lax
from jax.experimental import pallas as pl
from jax.experimental.pallas import tpu as pltpu
from jax.sharding import PartitionSpec as P

EPS = 1e-05
LANES = 128
TILE = 256
F32 = jnp.float32
MESH = pl.DeviceIdType.MESH


def bytes_of(ref, sem):
    return pltpu.make_async_copy(ref, ref, sem)


def stack(pieces):
    return pieces[0] if len(pieces) == 1 else jnp.concatenate(pieces, 0)


def kernel(n, nb, pair, owners, subs, stream, hidden, gain, weight, rewards, mask, lengths, horizon,
           out_ref,
           hv, gain_v, weight_v, rew_v, mask_v, len_s, hor_s,
           part, rbuf, rw_send, rw_recv, len_send, len_recv, hor_send, hor_recv,
           sum_send, sum_recv, tok_send, tok_recv, small_v, any_rows, held_squares,
           chunk_sem, small_sem, early, part_rs, late):
    R, T, depth = hidden.shape
    block = rewards.shape[1]
    width = block // nb
    per = n // owners
    base = (n - owners) // 2
    L = T // owners
    G = L // LANES
    gb = block // LANES
    rows = G * R
    Q = pair * R
    pairs = nb // pair
    total = depth * n
    s = lax.axis_index("seq")
    b = lax.axis_index("batch")
    side = b % pair
    mate = b // pair
    lead = mate * pair + pair - 1
    is_owner = (s >= base) & (s < base + owners) & (side == pair - 1)
    mine = s - base
    out_o = s // per
    half = s % per
    rw_at = base + out_o

    S = L // subs
    sent = small_sem.at[0]
    srows = rows // subs
    near_high = s * (owners // 2) // n
    near_low = s % 2

    def turn(k):
        back = owners - 1 - k
        if owners % 2:
            return (s + back) % owners
        return (near_high + back % (owners // 2)) % (owners // 2) * 2 + (near_low + back // (owners // 2)) % 2

    def chunk_copy(c, r=slice(None)):
        span = pl.ds(turn(c // subs) * L + c % subs * S, S)
        return pltpu.make_async_copy(hidden.at[r, span, :], hv.at[r, span, :], chunk_sem.at[c])

    def wait_rows(count, sem):
        if count:
            bytes_of(any_rows.at[pl.ds(0, count)], sem).wait()

    smalls = [
        pltpu.make_async_copy(src, dst, small_sem.at[i])
        for i, src, dst in ((0, gain, gain_v), (0, weight, weight_v), (0, rewards, rew_v),
                            (0, mask, mask_v), (1, lengths, len_s), (2, horizon, hor_s))]
    for c in range(owners * subs):
        for r in range(R):
            chunk_copy(c, r).start(priority=int(c > 0))
        if c == 0:
            for copy in smalls:
                copy.start()
    barrier = pltpu.get_barrier_semaphore()
    for k in range(1, nb):
        pl.semaphore_signal(barrier, inc=1, device_id={"batch": lax.rem(b + k, nb)},
                            device_id_type=MESH)

    @pl.when(is_owner)
    def _():
        for k in range(n):
            for c in range(pair):
                if k or c:
                    pl.semaphore_signal(
                        barrier, inc=1,
                        device_id={"seq": (s + k) % n, "batch": mate * pair + (side + c) % pair},
                        device_id_type=MESH)

    def head_pieces():
        head = (gain_v[...] * weight_v[...]).reshape(1, depth)
        high = head.astype(jnp.bfloat16).astype(F32)
        middle = (head - high).astype(jnp.bfloat16).astype(F32)
        low = head - high - middle
        wrow = lax.broadcasted_iota(jnp.int32, (16, depth), 0)
        pieces = jnp.where(wrow == 0, high, jnp.where(wrow == 1, middle, jnp.where(wrow == 2, low, 0.0)))
        return pieces.astype(jnp.bfloat16)

    def part_copy(o, j):
        return pltpu.make_async_remote_copy(
            part.at[o, j], rbuf.at[s * pair + side, j], sent, part_rs,
            device_id={"seq": base + o, "batch": lead}, device_id_type=MESH)

    def rw_copy():
        return pltpu.make_async_remote_copy(
            rw_send, rw_recv.at[side * per + half], sent, early,
            device_id={"seq": rw_at, "batch": lead}, device_id_type=MESH)

    def info_copy(k, src, dst):
        return pltpu.make_async_remote_copy(
            src, dst.at[b], sent, early,
            device_id={"batch": lax.rem(b + k, nb)}, device_id_type=MESH)

    infos = ((len_send, len_recv), (hor_send, hor_recv))
    own_rw = is_owner & (mine == out_o)

    def send_part(o, j):
        @pl.when(jnp.logical_not(is_owner & (mine == o)))
        def _():
            part_copy(o, j).start()

    bytes_of(small_v, small_sem.at[0]).wait()
    pieces = head_pieces()
    for copy in smalls[4:]:
        copy.wait()
    rw = rew_v[...] * mask_v[...].astype(F32)
    for g in range(gb):
        rw_send[g * R:(g + 1) * R, :] = rw[:, g * LANES:(g + 1) * LANES]
    for r in range(R):
        len_send[r:r + 1, :] = jnp.full((1, LANES), len_s[r], jnp.int32)
        hor_send[r:r + 1, :] = jnp.full((1, LANES), hor_s[r], F32)

    def enter():
        met = jnp.where(is_owner, owners - 1, owners) + nb - 1
        pl.semaphore_wait(barrier, met)

        @pl.when(jnp.logical_not(own_rw))
        def _():
            rw_copy().start()

        for j in range(1, nb):
            for src, dst in infos:
                info_copy(j, src, dst).start()

    def squares_of(h):
        squares = jnp.zeros((h.shape[0], LANES), F32)
        for j in range(depth // LANES):
            wide = h[:, j * LANES:(j + 1) * LANES].astype(F32)
            squares = squares + wide * wide
        return squares

    def compute(k, carry):
        o = turn(k)
        for j in range(subs):
            chunk_copy(k * subs + j).wait()
        for g in range(G):
            for r in range(R):
                at = pl.ds(pl.multiple_of(o * L + g * LANES, LANES), LANES)
                h = hv[r, at, :]
                sums = lax.dot_general(pieces, h, (((1,), (1,)), ((), ())),
                                       preferred_element_type=F32)
                j, row = divmod(g * R + r, srows)
                part[o, j, 0, row:row + 1, :] = jnp.sum(sums[0:8], 0, keepdims=True)
                part[o, j, 1, row:row + 1, :] = jnp.sum(squares_of(h).T, 0, keepdims=True)

        @pl.when(k == 0)
        def _():
            enter()

        for j in range(subs):
            send_part(o, j)
        return carry

    def streamed(*accs):
        for acc in accs:
            pltpu.matmul_pop(acc)
        for step in range(owners * subs + 1):
            if step < owners * subs:
                o, j = turn(step // subs), step % subs
                chunk_copy(step).wait()
                for r in range(R):
                    h = hv[r, pl.ds(pl.multiple_of(o * L + j * S, S), S), :]
                    for m in range(2):
                        cols = slice(m * TILE, (m + 1) * TILE)
                        pltpu.matmul_push_rhs(h[:, cols], staging_register=r, mxu_index=m,
                                              transpose=True)
                        pltpu.matmul_acc_lhs(accs[(step % 2 * R + r) * 2 + m], pieces[:, cols],
                                             load_staged_rhs=r)
                    held_squares[step % 2, r] = squares_of(h)
            if step == 0:
                enter()
            else:
                last = step - 1
                o, j = turn(last // subs), last % subs
                for r in range(R):
                    at = (last % 2 * R + r) * 2
                    sums = pltpu.matmul_pop(accs[at]) + pltpu.matmul_pop(accs[at + 1])
                    sums = jnp.sum(sums[0:8], 0, keepdims=True)
                    for g in range(S // LANES):
                        row = g * R + r
                        square = held_squares[last % 2, r, g * LANES:(g + 1) * LANES, :]
                        part[o, j, 0, row:row + 1, :] = sums[:, g * LANES:(g + 1) * LANES]
                        part[o, j, 1, row:row + 1, :] = jnp.sum(square.T, 0, keepdims=True)
                send_part(o, j)

    if stream:
        pl.run_scoped(streamed, *[pltpu.ACC(i % 2)((16, TILE), F32) for i in range(4 * R)])
    else:
        lax.fori_loop(0, owners, compute, 0)

    @pl.when(own_rw)
    def _():
        rw_recv[side * per + half] = rw_send[...]

    len_recv[b] = len_send[...]
    hor_recv[b] = hor_send[...]
    info_rows = 2 * R * (nb - 1)

    @pl.when(jnp.logical_not(is_owner))
    def _():
        wait_rows(info_rows, early)

    @pl.when(own_rw)
    def _():
        wait_rows(info_rows + gb * R * (pair * per - 1), early)

    @pl.when(is_owner & jnp.logical_not(own_rw))
    def _():
        wait_rows(info_rows + gb * R * pair * per, early)

    def sum_copy(i, j):
        return pltpu.make_async_remote_copy(
            sum_send, sum_recv.at[mine * pairs + mate], sent, late,
            device_id={"seq": i, "batch": j}, device_id_type=MESH)

    def each_sum():
        def one(i):
            for j in range(nb):
                never = isinstance(i, int) and not base <= i < base + owners
                if never or j % pair != pair - 1:
                    sum_copy(i, j).start()
                else:
                    @pl.when((i != s) | (j != b))
                    def _():
                        sum_copy(i, j).start()

        if n * nb <= 32:
            for i in range(n):
                one(i)
        else:
            def body(i, carry):
                one(i)
                return carry
            lax.fori_loop(0, n, body, 0)

    def tok_copy(h, j):
        return pltpu.make_async_remote_copy(
            tok_send.at[h * gb + (j * width) // LANES], tok_recv.at[mate], sent, late,
            device_id={"seq": mine * per + h, "batch": j}, device_id_type=MESH)

    @pl.when(is_owner)
    def _():
        row = lax.broadcasted_iota(jnp.int32, (pair * rows, LANES), 0)
        lane = lax.broadcasted_iota(jnp.int32, (pair * rows, LANES), 1)
        group = row % rows // R
        length = stack([len_recv[mate * pair + c] for c in range(pair) for _ in range(G)])
        reach = stack([hor_recv[mate * pair + c] for c in range(pair) for _ in range(G)])
        rate = -1.0 / reach
        local = group * LANES + lane
        valid = (mine * L + local < length).astype(F32)
        step = 12
        near = [jnp.where(lane < LANES - k, jnp.exp(rate * (k - 1)), 0.0) for k in range(1, step + 1)]
        far = [jnp.where(lane < LANES - k, jnp.exp(rate * k), 0.0) for k in range(step, LANES, step)]
        lead_in = jnp.exp(rate * lane.astype(F32))
        hops = [1 << i for i in range(max(G - 1, 0).bit_length())]
        row_decay = [jnp.where(group + k < G, jnp.exp(rate * (k * LANES)), 0.0) for k in hops]
        into = jnp.where(group < G - 1, jnp.exp(rate * (LANES - 1 - lane).astype(F32)), 0.0)
        power = jnp.exp(rate * (L - 1 - local).astype(F32))
        decay = jnp.exp(rate)
        gains = stack([rw_recv[c * per + h] for c in range(pair) for h in range(per)])

        rbuf[s * pair + side] = part[mine]
        bytes_of(rbuf.at[pl.ds(0, n * pair - 1)], part_rs).wait()
        projected, squares = [], []
        for c in range(pair):
            for j in range(subs):
                first, second = rbuf[c, j, 0], rbuf[c, j, 1]
                for k in range(1, n):
                    first = first + rbuf[k * pair + c, j, 0]
                    second = second + rbuf[k * pair + c, j, 1]
                projected.append(first)
                squares.append(second)
        values = stack(projected) * lax.rsqrt(stack(squares) / total + EPS)
        held = values * valid
        change = (gains - values) * valid
        mixed = decay * change + held
        start = jnp.sum(lead_in * mixed, 1, keepdims=True)
        terms = [factor * pltpu.roll(mixed if k < step else held, LANES - k, 1)
                 for k, factor in enumerate(near, 1)]
        while len(terms) > 1:
            terms = [sum(terms[i + 1:i + 2], terms[i]) for i in range(0, len(terms), 2)]
        gae = change + terms[0]
        terms = [factor * pltpu.roll(gae, LANES - k * step, 1) for k, factor in enumerate(far, 1)]
        while len(terms) > 1:
            terms = [sum(terms[i + 1:i + 2], terms[i]) for i in range(0, len(terms), 2)]
        gae = gae + terms[0]
        start = jnp.broadcast_to(start, gae.shape)
        if G > 1:
            for k, factor in zip(hops, row_decay):
                start = start + factor * pltpu.roll(start, pair * rows - k * R, 0)
            gae = gae + into * pltpu.roll(start, pair * rows - R, 0)
        sums = jnp.where(lane == 1, jnp.sum(gae, 1, keepdims=True), 0.0)
        sums = jnp.where(lane == 2, 2.0 * jnp.sum(gae * power, 1, keepdims=True), sums)
        sums = jnp.where(lane == 3, jnp.sum(gae * gae, 1, keepdims=True), sums)
        sums = jnp.where((lane == 0) & (group == 0), start, sums)
        if G & (G - 1) == 0:
            for k in hops:
                sums = sums + pltpu.roll(sums, pair * rows - k * R, 0)
            for c in range(pair):
                sum_send[c * R:(c + 1) * R, :] = sums[c * rows:c * rows + R]
        else:
            for c in range(pair):
                summary = sums[c * rows:c * rows + R]
                for g in range(1, G):
                    summary = summary + sums[c * rows + g * R:c * rows + (g + 1) * R]
                sum_send[c * R:(c + 1) * R, :] = summary
        each_sum()
        sum_recv[mine * pairs + mate] = sum_send[...]
        for g in range(G):
            for c in range(pair):
                at = c * rows + g * R
                tok_send[g, 0, c * R:(c + 1) * R, :] = gae[at:at + R]
                tok_send[g, 1, c * R:(c + 1) * R, :] = values[at:at + R]
        for h in range(per):
            for j in range(nb):
                if j % pair != pair - 1:
                    tok_copy(h, j).start()
                else:
                    @pl.when((mine * per + h != s) | (j != b))
                    def _():
                        tok_copy(h, j).start()

                    @pl.when((mine * per + h == s) & (j == b))
                    def _():
                        tok_recv[mate] = tok_send[h * gb + (j * width) // LANES]

    spots = LANES // width
    spot = b % spots

    def pick(x):
        result = x
        for j in range(1, spots):
            result = jnp.where(spot == j, pltpu.roll(x, LANES - j * width, 1), result)
        return result

    every = nb * R
    lane = lax.broadcasted_iota(jnp.int32, (every, LANES), 1)
    local = (half * gb + (b * width) // LANES) * LANES + lane
    length = stack([len_recv[c] for c in range(nb)])
    rate = -1.0 / stack([hor_recv[c] for c in range(nb)])
    count = jnp.sum(jnp.minimum(length, T).astype(F32), 0, keepdims=True)
    share = 1.0 / count
    jump = jnp.exp(rate * float(L))
    power_out = pick(jnp.exp(rate * (L - 1 - local).astype(F32)))
    valid_out = pick((out_o * L + local < length).astype(F32))
    power = [jnp.exp(rate * (L - 1 - g * LANES - lane).astype(F32)) for g in range(G)]
    power_sum = jnp.broadcast_to(jnp.sum(sum(power[1:], power[0]), 1, keepdims=True), (every, LANES))
    power = [x * x for x in power]
    power_squares = jnp.broadcast_to(jnp.sum(sum(power[1:], power[0]), 1, keepdims=True), (every, LANES))

    part_rows = 2 * rows * (owners - 1) + info_rows
    sum_rows = Q * owners * pairs
    tok_rows = 2 * Q * pairs

    @pl.when(jnp.logical_not(is_owner))
    def _():
        wait_rows(part_rows + 2 * rows + gb * R, sent)
        wait_rows(sum_rows + tok_rows, late)

    @pl.when(own_rw)
    def _():
        wait_rows(part_rows + Q * (n * nb - 1) + 2 * Q * (per * nb - 1), sent)
        wait_rows(sum_rows - Q + tok_rows - 2 * Q, late)

    @pl.when(is_owner & jnp.logical_not(own_rw))
    def _():
        wait_rows(part_rows + gb * R + Q * (n * nb - 1) + 2 * Q * per * nb, sent)
        wait_rows(sum_rows - Q + tok_rows, late)

    gae = pick(stack([tok_recv[c, 0] for c in range(pairs)]))
    values = pick(stack([tok_recv[c, 1] for c in range(pairs)]))
    messages = [stack([sum_recv[o * pairs + c] for c in range(pairs)]) for o in range(owners)]

    def spread(o, i):
        return jnp.broadcast_to(messages[o][:, i:i + 1], (every, LANES))

    u = spread(owners - 1, 0)
    first = sum([spread(o, 1) for o in range(1, owners)], spread(0, 1))
    second = sum([spread(o, 3) for o in range(1, owners)], spread(0, 3))
    entering = jnp.zeros((every, LANES), F32)
    for o in reversed(range(owners - 1)):
        first = first + u * power_sum
        second = second + u * (spread(o, 2) + u * power_squares)
        entering = jnp.where(out_o == o, u, entering)
        if o:
            u = spread(o, 0) + jump * u
    mean = jnp.sum(first, 0, keepdims=True) * share
    var = jnp.maximum(jnp.sum(second, 0, keepdims=True) * share - mean * mean, 1.0)
    scale = lax.rsqrt(var)
    gae = gae + power_out * entering
    out_ref[every:2 * every, :] = ((gae + values) * valid_out)[:, 0:width]
    out_ref[0:every, :] = ((gae - mean) * valid_out * scale)[:, 0:width]


def per_device(hidden, gain, weight, rewards, mask, lengths, horizon):
    n = lax.axis_size("seq")
    nb = lax.axis_size("batch")
    pair = 2 - nb % 2
    owners = n // 2 if n % 4 == 0 else n
    R, T, depth = hidden.shape
    subs = max(T // owners // TILE, 1)
    chunks = owners * subs
    stream = R == 2 and depth == 2 * TILE and T == chunks * TILE
    block = rewards.shape[1]
    per = n // owners
    G = T // owners // LANES
    gb = block // LANES
    rows = G * R
    Q = pair * R
    pairs = nb // pair
    dma = pltpu.SemaphoreType.DMA
    both = pl.pallas_call(
        functools.partial(kernel, n, nb, pair, owners, subs, stream),
        out_shape=pltpu.VMEM((2 * R * nb, block // nb), F32),
        in_specs=[pl.BlockSpec(memory_space=pl.ANY)] * 7,
        out_specs=pl.BlockSpec(memory_space=pltpu.VMEM),
        scratch_shapes=[
            pltpu.VMEM((R, T, depth), jnp.bfloat16),
            pltpu.VMEM((depth,), F32),
            pltpu.VMEM((depth,), F32),
            pltpu.VMEM((R, block), F32),
            pltpu.VMEM((R, block), jnp.int32),
            pltpu.SMEM((R,), jnp.int32),
            pltpu.SMEM((R,), F32),
            pltpu.VMEM((owners, subs, 2, rows // subs, LANES), F32),
            pltpu.VMEM((n * pair, subs, 2, rows // subs, LANES), F32),
            pltpu.VMEM((gb * R, LANES), F32),
            pltpu.VMEM((pair * per, gb * R, LANES), F32),
            pltpu.VMEM((R, LANES), jnp.int32),
            pltpu.VMEM((nb, R, LANES), jnp.int32),
            pltpu.VMEM((R, LANES), F32),
            pltpu.VMEM((nb, R, LANES), F32),
            pltpu.VMEM((Q, LANES), F32),
            pltpu.VMEM((owners * pairs, Q, LANES), F32),
            pltpu.VMEM((G, 2, Q, LANES), F32),
            pltpu.VMEM((pairs, 2, Q, LANES), F32),
            pltpu.VMEM((2 * depth + 2 * R * block,), F32),
            pltpu.VMEM((2 * owners * rows + 2 * R * nb + Q * n * nb + 2 * Q * per * nb + rows, LANES), F32),
            pltpu.VMEM((2, R, TILE, LANES), F32),
            dma((chunks,)), dma((3,)), dma(()), dma(()), dma(()),
        ],
        compiler_params=pltpu.CompilerParams(collective_id=0, has_side_effects=True),
    )(hidden, gain, weight, rewards, mask, lengths, horizon)
    return both[:R * nb], both[R * nb:]


def solution(mesh):
    return jax.shard_map(
        per_device,
        mesh=mesh,
        in_specs=(
            P("batch", None, "seq"),
            P("seq"),
            P("seq"),
            P("batch", "seq"),
            P("batch", "seq"),
            P("batch"),
            P("batch"),
        ),
        out_specs=(P(None, ("seq", "batch")), P(None, ("seq", "batch"))),
        check_vma=False,
    )
```
